128 devices in a mesh: seq: 32 (over x, z, core), head: 4 (over y).
Axes of the slice: x: 4, y: 4, z: 4, core: 2. Of those that a mesh axis runs over, the one named last changes fastest.
Arguments:
- inputs: bfloat16 [32768, 4096], P('seq', 'head'), may hold values from -6 to 6
- out_grad: bfloat16 [32768, 4096], P('seq', 'head'), may hold values from -6 to 6
- b_proj: bfloat16 [32768, 128], P('seq'), may hold values from -0.75 to 0.75
- c_proj: bfloat16 [32768, 128], P('seq'), may hold values from -3 to 3
- step_raw: float32 [32768, 64], P('seq', 'head'), may hold values from -3 to 12
- log_rate: float32 [64], P('head'), may hold values from -7 to -1.7
- step_bias: float32 [64], P('head'), may hold values from -7 to -1.6
- skip_gain: float32 [64], P('head'), may hold values from 0.5 to 1.5
- saved_states: float32 [32, 64, 64, 128], P(None, 'seq', 'head'), may hold values from -1.5 to 1.5
- segment_slot: int32 [32], replicated, may hold values from 0 to 31, each once
Outputs:
- grad_inputs: bfloat16 [32768, 4096], P('seq', 'head')
- grad_step_raw: float32 [32768, 64], P('seq', 'head')
- grad_b: float32 [32768, 128], P(('seq', 'head'))
- grad_c: float32 [32768, 128], P(('seq', 'head'))
The draws below stay inside these ranges and needn't reach their ends.
Inputs may be any that keep to these rules, and one draw needn't show every extreme that they name: `segment_slot`: a permutation of the segments.
All inputs are finite; a program needn't handle non-finite values.
Results may differ from the reference program's by a relative error of at most 0.0012.
Values sent between devices are 32-bit elements; how exact they have to be, the bound alone decides.
No kernel may reach another device: no remote copies, remote signals or barrier semaphores. Data moves between devices by JAX's collectives and lax.ppermute only.
A program may use at most 128 MiB of HBM per device.

```python
import jax
import jax.numpy as jnp
from jax import lax

H = 64
P_SIZE = 64
N = 128
SPAN = 256
TOK_DEV = 1024
SEGS = 32
TOKEN_COUNT = 32768


def head_rates(key):
    rate_key = jax.random.fold_in(key, 11)
    lowest = jnp.log(0.5 / TOKEN_COUNT)
    highest_rate = jnp.log(1.0 / 30.0)
    uniform_part = jax.random.uniform(rate_key, (H,), jnp.float32)
    log_value = lowest + uniform_part * (highest_rate - lowest)
    return jnp.exp(0.5 * log_value)


def draw_log_rate(key, part):
    return jnp.log(head_rates(key)).astype(jnp.float32)


def draw_step_bias(key, part):
    return jnp.log(jnp.expm1(head_rates(key))).astype(jnp.float32)


def draw_step_raw(key, part):
    private_random_key = jax.random.fold_in(key, 21)
    jitter_random_key, offset_random_key, spike_random_key = jax.random.split(private_random_key, 3)
    random_jitter = 0.5 * jnp.clip(jax.random.normal(jitter_random_key, (TOKEN_COUNT, H), jnp.float32), -3.0, 3.0)
    shifts = jax.random.uniform(offset_random_key, (SEGS, 1, H), jnp.float32, -0.7, 0.7)
    random_jitter = (random_jitter.reshape(SEGS, TOK_DEV, H) + shifts).reshape(TOKEN_COUNT, H)
    spike_positions = jax.random.randint(spike_random_key, (3,), 0, TOKEN_COUNT)
    spike_values = jnp.any(jnp.arange(TOKEN_COUNT)[:, None] == spike_positions[None, :], axis=1)
    return (random_jitter + 9.0 * spike_values[:, None].astype(jnp.float32)).astype(jnp.float32)


def shard_levels(own_key, extent, cuts, least, high):
    def one(position, shards_of):
        draws = jax.random.uniform(jax.random.fold_in(jax.random.fold_in(own_key, 6), position), (shards_of,), jnp.float32, least / len(cuts), high / len(cuts))
        return jnp.repeat(jnp.exp(draws), extent[position] // shards_of).reshape((-1,) + (1,) * (len(extent) - position - 1))

    gain = one(*cuts[0])
    for cut in cuts[1:]:
        gain = gain * one(*cut)
    return gain


def scatter_about(rng, shape, scale, bound, cuts=(), held_as=jnp.bfloat16):
    array = jax.random.normal(rng, shape, jnp.float32) * scale
    if len(cuts) > 0:
        array = shard_levels(rng, shape, cuts, -0.22, 0.18) * array
    return jnp.clip(array, min=-bound, max=bound).astype(held_as)


def setup_inputs(seed: int = 0) -> dict:
    streams_of = jax.random.split(jax.random.key(seed), 11)
    return {
        "inputs": scatter_about(streams_of[0], (TOKEN_COUNT, H * P_SIZE), 1.0, 6.0, ((0, 32), (1, 4))),
        "out_grad": scatter_about(streams_of[1], (TOKEN_COUNT, H * P_SIZE), 1.0, 6.0, ((0, 32), (1, 4))),
        "b_proj": scatter_about(streams_of[2], (TOKEN_COUNT, N), 0.125, 0.75, ((0, 32),)),
        "c_proj": scatter_about(streams_of[3], (TOKEN_COUNT, N), 0.5, 3.0, ((0, 32),)),
        "step_raw": draw_step_raw(jax.random.fold_in(streams_of[10], 71), 0),
        "log_rate": draw_log_rate(jax.random.fold_in(streams_of[10], 71), 0),
        "step_bias": draw_step_bias(jax.random.fold_in(streams_of[10], 71), 0),
        "skip_gain": jnp.clip(0.5 + 1.0 * jax.random.uniform(streams_of[7], (H,), jnp.float32) ** shard_levels(streams_of[7], (H,), ((0, 4),), -0.2, 0.2), 0.5, 1.5),
        "saved_states": scatter_about(streams_of[8], (SEGS, H, P_SIZE, N), 0.25, 1.5, ((1, 32), (2, 4)), jnp.float32),
        "segment_slot": jax.random.permutation(streams_of[9], SEGS).astype(jnp.int32),
    }


highest = lax.Precision.HIGHEST

def block_forward(carried, item, decay_rate, skip_gain, start_states, per_segment):
    block_index, input_block, b_block, c_block, step_block = item
    start = lax.dynamic_index_in_dim(start_states, block_index // per_segment, 0, keepdims=False)
    opening = block_index % per_segment == 0
    entering = jnp.where(opening, start + carried - lax.stop_gradient(carried), carried)
    log_decay = -decay_rate[None, :] * step_block
    cumulative = jnp.cumsum(log_decay, axis=0)
    positions = jnp.arange(cumulative.shape[0])
    lower_mask = positions[:, None] >= positions[None, :]
    spread = cumulative.T[:, :, None] - cumulative.T[:, None, :]
    decay = jnp.where(lower_mask, jnp.exp(jnp.where(lower_mask, spread, 0.0)), 0.0)
    intersection = jnp.einsum('tn,un->tu', c_block, b_block, precision=highest)
    weights = decay * intersection[None, :, :] * step_block.T[:, None, :]
    outputs = jnp.einsum('htu,uhp->thp', weights, input_block, precision=highest)
    outputs = outputs + jnp.exp(cumulative)[:, :, None] * jnp.einsum('hpn,tn->thp', entering, c_block, precision=highest)
    outputs = outputs + skip_gain[None, :, None] * input_block
    block_end = cumulative[-1]
    to_end = jnp.exp(block_end[None, :] - cumulative) * step_block
    leaving = jnp.exp(block_end)[:, None, None] * entering + jnp.einsum('uhp,un->hpn', input_block * to_end[:, :, None], b_block, precision=highest)
    return (leaving, outputs)

def reference(inputs, out_grad, b_proj, c_proj, step_raw, log_rate, step_bias, skip_gain, saved_states, segment_slot):
    seg_count = saved_states.shape[0]
    inverse_order = jnp.zeros((seg_count,), jnp.int32).at[segment_slot].set(jnp.arange(seg_count, dtype=jnp.int32))
    start_states = jnp.take(saved_states, inverse_order, axis=0)
    tok_count, state_dim = b_proj.shape
    head_count = step_raw.shape[1]
    head_width = inputs.shape[1] // head_count
    block_count = tok_count // SPAN
    per_segment = TOK_DEV // SPAN
    decay_rate = jnp.exp(log_rate)

    def forward(input_full, b_full, c_full, raw_full):
        step_size = jax.nn.softplus(raw_full + step_bias[None, :])

        def advance(carried, item):
            return block_forward(carried, item, decay_rate, skip_gain, start_states, per_segment)
        items = (jnp.arange(block_count, dtype=jnp.int32), input_full.reshape(block_count, SPAN, head_count, head_width), b_full.reshape(block_count, SPAN, state_dim), c_full.reshape(block_count, SPAN, state_dim), step_size.reshape(block_count, SPAN, head_count))
        initial = jnp.zeros((head_count, head_width, state_dim), jnp.float32)
        unused_end, outputs = lax.scan(jax.checkpoint(advance), initial, items)
        return outputs.reshape(tok_count, head_count * head_width)
    primals = (inputs.astype(jnp.float32), b_proj.astype(jnp.float32), c_proj.astype(jnp.float32), step_raw)
    unused_out, pullback = jax.vjp(forward, *primals)
    grad_inputs, grad_b, grad_c, grad_raw = pullback(out_grad.astype(jnp.float32))
    return (grad_inputs.astype(jnp.bfloat16), grad_raw, grad_b, grad_c)
```

```python
import jax
import jax.numpy as jnp
from jax import lax
from jax.experimental import pallas as pl
from jax.experimental.pallas import tpu as pltpu
from jax.sharding import PartitionSpec as P

f32 = jnp.float32
bf16 = jnp.bfloat16
Q = 128
LOG2E = 1.4426950408889634
HIGHEST = lax.Precision.HIGHEST


def dn(a, b, precision=None):
    return lax.dot_general(
        a, b, (((1,), (0,)), ((), ())), precision=precision, preferred_element_type=f32
    )


def dt(a, b, precision=None):
    return lax.dot_general(
        a, b, (((1,), (1,)), ((), ())), precision=precision, preferred_element_type=f32
    )


def split(value):
    high = value.astype(bf16)
    low = (value - high.astype(f32)).astype(bf16)
    return high, low


def side(*parts):
    return jnp.concatenate(parts, axis=1)


def stack(*parts):
    return jnp.concatenate(parts, axis=0)


def spread(cols, base):
    rows = cols.shape[0]
    first = lax.broadcasted_iota(jnp.int32, (rows, 128), 1) < 64
    parts = []
    for j in range(2):
        left, right = (
            jnp.broadcast_to(cols[:, k : k + 1], (rows, 128))
            for k in (base + 2 * j, base + 2 * j + 1)
        )
        parts.append(jnp.where(first, left, right))
    return side(*parts)


def group_cols(cols, group):
    return pltpu.roll(cols, (128 - 4 * group) % 128, 1)


def head_sums(product, at):
    row = lax.broadcasted_iota(jnp.int32, (8, 256), 0)
    lane = lax.broadcasted_iota(jnp.int32, (8, 256), 1)
    pick = jnp.where(row - at == lane // 64, 1.0, 0.0).astype(bf16)
    high, low = split(product)
    return dt(side(pick, pick), side(high, low))


LOGCOL, GROW, SHRINK, GROW_ALL, SHRINK_ALL, SKIP = (16 * q for q in range(6))


def first_kernel(
    raw_ref, par_ref, dy_ref, b_ref, c_ref,
    sums_ref, cols_ref, info_ref, bt_ref, ct_ref, pad_ref,
):
    blocks = raw_ref.shape[0] // Q
    pad_ref[:, 0:16] = raw_ref[...] + par_ref[1:2, :]
    turned = pad_ref[...].T
    pad_ref[0:8, 0:16] = jnp.broadcast_to(jnp.exp(par_ref[0:1, :]), (8, 16))
    pad_ref[8:16, 0:16] = jnp.broadcast_to(par_ref[2:3, :], (8, 16))
    small = pad_ref[0:Q, :].T
    rate = jnp.broadcast_to(small[0:16, 0:1], (16, Q))
    skip = jnp.broadcast_to(small[0:16, 8:9], (16, Q))
    upper = jnp.where(
        lax.broadcasted_iota(jnp.int32, (Q, Q), 0) <= lax.broadcasted_iota(jnp.int32, (Q, Q), 1),
        1.0, 0.0,
    )
    steps, gates, decays = [], [], []
    for k in range(blocks):
        z = turned[0:16, k * Q : (k + 1) * Q]
        small_exp = jnp.exp(-jnp.abs(z))
        step = jnp.maximum(z, 0.0) + jnp.log1p(small_exp)
        gates.append(jnp.where(z >= 0.0, 1.0, small_exp) / (1.0 + small_exp))
        steps.append(step)
        decays.append(-rate * step * LOG2E)
    sums = dn(stack(*decays), upper, HIGHEST)
    logs = [sums[16 * k : 16 * k + 16] for k in range(blocks)]
    ends = [log[:, Q - 1 : Q] for log in logs]
    total = ends[0]
    for end in ends[1:]:
        total = total + end
    so_far = jnp.zeros_like(total)
    fill = jnp.zeros((32, Q), f32)
    for k in range(blocks):
        log, step = logs[k], steps[k]
        whole = log + so_far
        so_far = so_far + ends[k]
        cols_ref[k * Q : (k + 1) * Q, :] = stack(
            log - jnp.log(step) * LOG2E,
            jnp.exp2(log),
            step * jnp.exp2(ends[k] - log),
            jnp.exp2(whole),
            step * jnp.exp2(total - whole),
            skip,
            fill,
        ).T
        for g in range(4):
            four = slice(4 * g, 4 * g + 4)
            info_ref[g, :, k * Q : (k + 1) * Q] = stack(
                log[four], step[four], gates[k][four], rate[four]
            )
        ct_ref[k] = c_ref[k * Q : (k + 1) * Q, :].astype(f32).T.astype(bf16)
        bt_ref[k] = b_ref[k * Q : (k + 1) * Q, :].astype(f32).T.astype(bf16)
    zero_rows = jnp.zeros((4, 128), f32)
    ends_row = []
    for g in range(4):

        def add(k, acc, g=g):
            rows = pl.ds(pl.multiple_of(k * Q, Q), Q)
            grow = spread(cols_ref[rows, :], GROW_ALL + 4 * g)
            high, low = split(dy_ref[rows, 256 * g : 256 * g + 256].astype(f32) * grow)
            ct = ct_ref[k]
            return acc + dn(side(ct, ct), stack(high, low))

        acc = lax.fori_loop(0, blocks, add, jnp.zeros((128, 256), f32))
        at = (g % 2) * 256
        for i in range(16):
            sums_ref[2 * i + g // 2, :, at : at + 256] = acc[8 * i : 8 * i + 8]
        last = spread(cols_ref[blocks * Q - 8 : blocks * Q, :], GROW_ALL + 4 * g)[7:8, :]
        ends_row += [last[:, 0:128], last[:, 128:256]]
    for half in range(2):
        tile = stack(*ends_row[4 * half : 4 * half + 4], zero_rows)
        for i in range(16):
            sums_ref[2 * i + half, :, 512:640] = tile


def order_kernel(slot_ref, saved_ref, out_ref):
    for k in range(saved_ref.shape[0]):
        out_ref[slot_ref[k]] = saved_ref[k]


def carry_kernel(sums_ref, out_ref):
    carried = jnp.zeros((8, 512), f32)
    for m in reversed(range(sums_ref.shape[0])):
        out_ref[m] = carried
        decay = side(
            *[jnp.broadcast_to(sums_ref[m, r : r + 1, 512:640], (8, 128)) for r in range(4)]
        )
        carried = sums_ref[m, :, 0:512] + decay * carried


def local_kernel(
    x_ref, dy_ref, b_ref, c_ref, bt_ref, ct_ref, cols_ref, info_ref,
    adj_ref, gb_ref, gc_ref, rx_ref,
    state_ref, high_ref, low_ref, tot_ref,
):
    g = pl.program_id(0)
    blocks = x_ref.shape[0] // Q

    @pl.when(g == 0)
    def clear():
        gb_ref[...] = jnp.zeros_like(gb_ref)
        gc_ref[...] = jnp.zeros_like(gc_ref)
        tot_ref[...] = jnp.zeros_like(tot_ref)

    def rows_of(k):
        return pl.ds(pl.multiple_of(k * Q, Q), Q)

    def forward(k, state):
        rows = rows_of(k)
        cols = group_cols(cols_ref[rows, :], g)
        state_ref[k] = state
        high, low = split(x_ref[rows, :].astype(f32) * spread(cols, SHRINK))
        high_ref[rows, :] = high
        low_ref[rows, :] = low
        bt = bt_ref[k]
        decay = spread(cols[Q - 8 : Q, :], GROW)[7:8, :]
        return decay * state + dn(side(bt, bt), stack(high, low))

    lax.fori_loop(0, blocks, forward, jnp.zeros((128, 256), f32))
    skip = spread(group_cols(cols_ref[0:8, :], g), SKIP)[0:1, :]
    upper = lax.broadcasted_iota(jnp.int32, (Q, Q), 0) <= lax.broadcasted_iota(
        jnp.int32, (Q, Q), 1
    )
    lane = lax.broadcasted_iota(jnp.int32, (1, 128), 1)
    masks = [jnp.where(lane < 64, 1.0, 0.0).astype(bf16), jnp.where(lane < 64, 0.0, 1.0).astype(bf16)]

    def backward(step, adjoint):
        k = blocks - 1 - step
        rows = rows_of(k)
        cols = group_cols(cols_ref[rows, :], g)
        b, c, ct = b_ref[rows, :], c_ref[rows, :], ct_ref[k]
        x, dy = x_ref[rows, :], dy_ref[rows, :]
        x_full, dy_full = x.astype(f32), dy.astype(f32)
        grow = spread(cols, GROW)
        dy_grown = dy_full * grow
        dy_high, dy_low = split(dy_grown)
        s_high, s_low = split(state_ref[k])
        g_high, g_low = split(adjoint)
        meet = dt(b, c)
        from_state = dn(side(c, c), stack(s_high, s_low))
        from_right = spread(cols, SHRINK) * dn(side(b, b), stack(g_high, g_low))
        pieces, in_rows = [], []
        total = tot_ref[k]
        for j in range(2):
            x_pair = x[:, 128 * j : 128 * j + 128]
            dy_pair = dy[:, 128 * j : 128 * j + 128]
            weights, values = [], []
            for i in range(2):
                h = 2 * j + i
                log_row = info_ref[0, h : h + 1, rows]
                gap = log_row - jnp.broadcast_to(cols[:, LOGCOL + h : LOGCOL + h + 1], (Q, Q))
                decay = jnp.exp2(jnp.where(upper, gap, -1e30))
                pair = dt(x_pair * masks[i], dy_pair) * decay
                total = total + pair
                in_rows.append(jnp.sum(pair * meet, axis=0, keepdims=True))
                weights += list(split(decay * meet))
                values += [dy_pair * masks[i]] * 2
            pieces.append(dn(side(*weights), stack(*values)))
        tot_ref[k] = total
        adj = side(*pieces) + from_right
        adj_ref[rows, :] = adj + skip * dy_full
        out_part = x_full * adj
        in_part = dy_grown * from_state
        rx_ref[0, :, rows] = (
            head_sums(in_part - out_part, 0)
            + head_sums(out_part, 4)
            + stack(*in_rows, jnp.zeros((4, Q), f32))
        )
        gc_ref[rows, :] += dt(side(dy_high, dy_low, dy_high), side(s_high, s_high, s_low))
        x_high, x_low = high_ref[rows, :], low_ref[rows, :]
        gb_ref[rows, :] += dt(side(x_high, x_low, x_high), side(g_high, g_high, g_low))
        return grow[Q - 1 : Q, :] * adjoint + dn(side(ct, ct), stack(dy_high, dy_low))

    lax.fori_loop(0, blocks, backward, jnp.zeros((128, 256), f32))

    @pl.when(g == pl.num_programs(0) - 1)
    def finish():
        for k in range(blocks):
            rows = slice(k * Q, (k + 1) * Q)
            total = tot_ref[k]
            high, low = split(total)
            c = c_ref[rows, :]
            gb_ref[rows, :] += dn(side(high, low), stack(c, c))
            high, low = split(total.T)
            b = b_ref[rows, :]
            gc_ref[rows, :] += dn(side(high, low), stack(b, b))


def start_kernel(
    dy_ref, c_ref, cols_ref, start_ref, gc_in_ref, gc_ref, rs_ref, turned_ref, hold_ref
):
    g = pl.program_id(0)
    blocks = dy_ref.shape[0] // Q

    @pl.when(g == 0)
    def copy():
        gc_ref[...] = gc_in_ref[...]

    for h in range(4):
        for q in range(4):
            hold_ref[64 * h + 16 * q : 64 * h + 16 * q + 16, :] = start_ref[q, h]
    start = hold_ref[...].T
    turned_ref[...] = start
    s_high, s_low = split(start)

    def one(k, unused):
        rows = pl.ds(pl.multiple_of(k * Q, Q), Q)
        grow = spread(group_cols(cols_ref[rows, :], g), GROW_ALL)
        c = c_ref[rows, :]
        dy_grown = dy_ref[rows, :].astype(f32) * grow
        dy_high, dy_low = split(dy_grown)
        from_state = dn(side(c, c), stack(s_high, s_low))
        rs_ref[0, :, rows] = head_sums(dy_grown * from_state, 0)
        gc_ref[rows, :] += dt(side(dy_high, dy_low, dy_high), side(s_high, s_high, s_low))
        return unused

    lax.fori_loop(0, blocks, one, 0)


def last_kernel(
    x_ref, b_ref, cols_ref, info_ref, adj_ref, gb_in_ref, rx_ref, rs_ref, turned_ref, in_ref,
    gx_ref, gb_ref, raw_ref, grad_ref, pad_ref,
):
    g = pl.program_id(0)
    blocks = x_ref.shape[0] // Q

    @pl.when(g == 0)
    def copy():
        gb_ref[...] = gb_in_ref[...]

    incoming = in_ref[...].reshape(128, 256)
    g_high, g_low = split(incoming)

    def one(k, unused):
        rows = pl.ds(pl.multiple_of(k * Q, Q), Q)
        shrink = spread(group_cols(cols_ref[rows, :], g), SHRINK_ALL)
        b = b_ref[rows, :]
        x_full = x_ref[rows, :].astype(f32)
        adj = shrink * dn(side(b, b), stack(g_high, g_low))
        gx_ref[rows, :] = (adj_ref[rows, :] + adj).astype(bf16)
        grad_ref[g, :, rows] = head_sums(x_full * adj, 0)
        x_high, x_low = split(x_full * shrink)
        gb_ref[rows, :] += dt(side(x_high, x_low, x_high), side(g_high, g_high, g_low))
        return unused

    lax.fori_loop(0, blocks, one, 0)
    last = spread(group_cols(cols_ref[blocks * Q - 8 : blocks * Q, :], g), GROW_ALL)[7:8, :]
    cross = last * jnp.sum(incoming * turned_ref[...], axis=0, keepdims=True)
    row = lax.broadcasted_iota(jnp.int32, (8, 256), 0)
    lane = lax.broadcasted_iota(jnp.int32, (8, 256), 1)
    through = jnp.sum(jnp.where(row == lane // 64, cross, 0.0), axis=1, keepdims=True)
    one_way = lax.broadcasted_iota(jnp.int32, (Q, Q), 0)
    other = lax.broadcasted_iota(jnp.int32, (Q, Q), 1)
    before = jnp.where(one_way < other, 1.0, 0.0)
    after = jnp.where(one_way >= other, 1.0, 0.0)
    ins, outs = [], []
    for k in range(blocks):
        rows = slice(k * Q, (k + 1) * Q)
        ins.append(rx_ref[0, :, rows] + rs_ref[0, :, rows])
        outs.append(grad_ref[g, :, rows])
    in_sums = dn(stack(*ins), after, HIGHEST)
    out_sums = dn(stack(*outs), before, HIGHEST)
    later = jnp.zeros((8, 1), f32)
    laters = []
    for k in reversed(range(blocks)):
        laters.insert(0, later)
        later = later + in_sums[8 * k : 8 * k + 8, 0:1]
    earlier = through
    for k in range(blocks):
        rows = slice(k * Q, (k + 1) * Q)
        decay_grad = in_sums[8 * k : 8 * k + 8] + laters[k] + out_sums[8 * k : 8 * k + 8] + earlier
        earlier = earlier + out_sums[8 * k : 8 * k + 8, Q - 1 : Q] + outs[k][:, Q - 1 : Q]
        step, gate, rate = (info_ref[0, 4 * r : 4 * r + 4, rows] for r in (1, 2, 3))
        x_adj = rx_ref[0, 4:8, rows] + outs[k][0:4]
        grad_ref[g, 0:4, rows] = gate * (x_adj / step - rate * decay_grad[0:4])

    @pl.when(g == pl.num_programs(0) - 1)
    def finish():
        for r in range(4):
            pad_ref[4 * r : 4 * r + 4, :] = grad_ref[r, 0:4, :]
        raw_ref[...] = pad_ref[...].T[:, 0:16]


def whole(shape):
    zeros = (0,) * len(shape)
    return pl.BlockSpec(tuple(shape), lambda g, zeros=zeros: zeros)


def on_device(
    inputs, out_grad, b_proj, c_proj, step_raw, log_rate, step_bias, skip_gain,
    saved_states, segment_slot,
):
    tok = inputs.shape[0]
    blocks = tok // Q
    segs = saved_states.shape[0]
    arbitrary = pltpu.CompilerParams(dimension_semantics=("arbitrary",))
    params = jnp.stack([log_rate, step_bias, skip_gain])
    sums, cols, info, bt, ct = pl.pallas_call(
        first_kernel,
        out_shape=(
            jax.ShapeDtypeStruct((segs, 8, 640), f32),
            jax.ShapeDtypeStruct((tok, 128), f32),
            jax.ShapeDtypeStruct((4, 16, tok), f32),
            jax.ShapeDtypeStruct((blocks, 128, Q), bf16),
            jax.ShapeDtypeStruct((blocks, 128, Q), bf16),
        ),
        scratch_shapes=[pltpu.VMEM((tok, 128), f32)],
        cost_estimate=pl.CostEstimate(flops=10**9, transcendentals=10**5, bytes_accessed=4 * 10**6),
        name="first",
    )(step_raw, params, out_grad, b_proj, c_proj)
    sums = lax.all_to_all(sums, "seq", split_axis=0, concat_axis=0, tiled=True)
    ordered = pl.pallas_call(
        order_kernel,
        out_shape=jax.ShapeDtypeStruct(saved_states.shape, f32),
        in_specs=[pl.BlockSpec(memory_space=pltpu.SMEM), pl.BlockSpec(memory_space=pltpu.VMEM)],
        out_specs=pl.BlockSpec(memory_space=pltpu.VMEM),
        name="order",
    )(segment_slot, saved_states)
    start = lax.all_to_all(ordered, "seq", split_axis=0, concat_axis=0, tiled=True)
    start = lax.all_to_all(
        start.reshape(4, 16, 16, 128), "head", split_axis=0, concat_axis=0, tiled=True
    )
    half = pl.BlockSpec((tok, 256), lambda g: (0, g))
    narrow = whole((tok, 128))
    rows8 = pl.BlockSpec((1, 8, tok), lambda g: (g, 0, 0))
    info_spec = pl.BlockSpec((1, 16, tok), lambda g: (g, 0, 0))
    turn = whole((blocks, 128, Q))
    adj, gb_local, gc_local, rx = pl.pallas_call(
        local_kernel,
        grid=(4,),
        in_specs=[half, half, narrow, narrow, turn, turn, narrow, info_spec],
        out_specs=[half, narrow, narrow, rows8],
        out_shape=(
            jax.ShapeDtypeStruct((tok, 1024), f32),
            jax.ShapeDtypeStruct((tok, 128), f32),
            jax.ShapeDtypeStruct((tok, 128), f32),
            jax.ShapeDtypeStruct((4, 8, tok), f32),
        ),
        scratch_shapes=[
            pltpu.VMEM((blocks, 128, 256), f32),
            pltpu.VMEM((tok, 256), bf16),
            pltpu.VMEM((tok, 256), bf16),
            pltpu.VMEM((blocks, Q, Q), f32),
        ],
        compiler_params=arbitrary,
        cost_estimate=pl.CostEstimate(
            flops=2 * 10**10, transcendentals=4 * 10**6, bytes_accessed=10**7
        ),
        name="local",
    )(inputs, out_grad, b_proj, c_proj, bt, ct, cols, info)
    carried = pl.pallas_call(
        carry_kernel,
        out_shape=jax.ShapeDtypeStruct((segs, 8, 512), f32),
        cost_estimate=pl.CostEstimate(flops=10**6, transcendentals=0, bytes_accessed=10**6),
        name="carry",
    )(sums)
    incoming = lax.all_to_all(carried, "seq", split_axis=0, concat_axis=0, tiled=True)
    gc, rs, turned = pl.pallas_call(
        start_kernel,
        grid=(4,),
        in_specs=[
            half, narrow, narrow,
            pl.BlockSpec((4, 4, 16, 128), lambda g: (0, g, 0, 0)), narrow,
        ],
        out_specs=[narrow, rows8, pl.BlockSpec((128, 256), lambda g: (0, g))],
        out_shape=(
            jax.ShapeDtypeStruct((tok, 128), f32),
            jax.ShapeDtypeStruct((4, 8, tok), f32),
            jax.ShapeDtypeStruct((128, 1024), f32),
        ),
        scratch_shapes=[pltpu.VMEM((256, 128), f32)],
        compiler_params=arbitrary,
        cost_estimate=pl.CostEstimate(
            flops=3 * 10**9, transcendentals=0, bytes_accessed=5 * 10**6
        ),
        name="start",
    )(out_grad, c_proj, cols, start, gc_local)
    gc = lax.all_to_all(
        gc.reshape(4, tok // 4, 128), "head", split_axis=0, concat_axis=0, tiled=True
    ).sum(axis=0)
    grad_inputs, gb, grad_step_raw = pl.pallas_call(
        last_kernel,
        grid=(4,),
        in_specs=[
            half, narrow, narrow, info_spec, half, narrow, rows8, rows8,
            pl.BlockSpec((128, 256), lambda g: (0, g)),
            pl.BlockSpec((16, 1, 8, 256), lambda g: (0, g // 2, 0, g % 2)),
        ],
        out_specs=[half, narrow, whole((tok, 16))],
        out_shape=(
            jax.ShapeDtypeStruct((tok, 1024), bf16),
            jax.ShapeDtypeStruct((tok, 128), f32),
            jax.ShapeDtypeStruct((tok, 16), f32),
        ),
        scratch_shapes=[pltpu.VMEM((4, 8, tok), f32), pltpu.VMEM((128, tok), f32)],
        compiler_params=arbitrary,
        cost_estimate=pl.CostEstimate(
            flops=3 * 10**9, transcendentals=0, bytes_accessed=10**7
        ),
        name="last",
    )(
        inputs, b_proj, cols, info, adj, gb_local, rx, rs, turned,
        incoming.reshape(16, 2, 8, 512),
    )
    gb = lax.all_to_all(
        gb.reshape(4, tok // 4, 128), "head", split_axis=0, concat_axis=0, tiled=True
    ).sum(axis=0)
    return grad_inputs, grad_step_raw, gb, gc


def solution(mesh):
    return jax.shard_map(
        on_device,
        mesh=mesh,
        in_specs=(
            P("seq", "head"),
            P("seq", "head"),
            P("seq", None),
            P("seq", None),
            P("seq", "head"),
            P("head"),
            P("head"),
            P("head"),
            P(None, "seq", "head", None),
            P(),
        ),
        out_specs=(P("seq", "head"), P("seq", "head"), P(("seq", "head"), None), P(("seq", "head"), None)),
        check_vma=False,
    )
```

```python
import jax
import jax.numpy as jnp
from jax import lax
from jax.experimental import pallas as pl
from jax.experimental.pallas import tpu as pltpu
from jax.sharding import PartitionSpec as P

f32 = jnp.float32
bf16 = jnp.bfloat16
Q = 128
LOG2E = 1.4426950408889634
HIGHEST = lax.Precision.HIGHEST


def dn(a, b, precision=None):
    return lax.dot_general(
        a, b, (((1,), (0,)), ((), ())), precision=precision, preferred_element_type=f32
    )


def dt(a, b, precision=None):
    return lax.dot_general(
        a, b, (((1,), (1,)), ((), ())), precision=precision, preferred_element_type=f32
    )


def split(value):
    high = value.astype(bf16)
    low = (value - high.astype(f32)).astype(bf16)
    return high, low


def side(*parts):
    return jnp.concatenate(parts, axis=1)


def stack(*parts):
    return jnp.concatenate(parts, axis=0)


def spread(cols, base):
    rows = cols.shape[0]
    first = lax.broadcasted_iota(jnp.int32, (rows, 128), 1) < 64
    parts = []
    for j in range(2):
        left, right = (
            jnp.broadcast_to(cols[:, k : k + 1], (rows, 128))
            for k in (base + 2 * j, base + 2 * j + 1)
        )
        parts.append(jnp.where(first, left, right))
    return side(*parts)


def group_cols(cols, group):
    return pltpu.roll(cols, (128 - 4 * group) % 128, 1)


def head_sums(product):
    rows = []
    for j in range(2):
        turned = product[:, 128 * j : 128 * j + 128].T
        for i in range(2):
            part = turned[64 * i : 64 * i + 64]
            eight = part[0:8]
            for r in range(1, 8):
                eight = eight + part[8 * r : 8 * r + 8]
            rows.append(jnp.sum(eight, axis=0, keepdims=True))
    return stack(*rows)


LOGCOL, GROW, SHRINK, GROW_ALL, SKIP = (16 * q for q in range(5))


def first_kernel(
    slot_ref, raw_ref, par_ref, dy_ref, b_ref, c_ref, saved_ref,
    sums_ref, cols_ref, info_ref, bt_ref, high_ref, low_ref, delta_ref,
    pad_ref, ct_ref,
):
    g = pl.program_id(0)
    blocks = dy_ref.shape[0] // Q

    @pl.when(g == 0)
    def prepare():
        for k in range(saved_ref.shape[0]):
            sums_ref[slot_ref[k], 40:72, :] = saved_ref[k]
        pad_ref[0:8, :] = jnp.broadcast_to(jnp.exp(par_ref[0:1, :]), (8, 128))
        pad_ref[8:16, :] = jnp.broadcast_to(par_ref[1:2, :], (8, 128))
        pad_ref[16:24, :] = jnp.broadcast_to(par_ref[2:3, :], (8, 128))
        small = pad_ref[...].T
        rate, bias, skip = (
            jnp.broadcast_to(small[0:16, k : k + 1], (16, Q)) for k in (0, 8, 16)
        )
        row = lax.broadcasted_iota(jnp.int32, (Q, Q), 0)
        lane = lax.broadcasted_iota(jnp.int32, (Q, Q), 1)
        upper = jnp.where(row <= lane, 1.0, 0.0)
        steps, gates, decays = [], [], []
        for k in range(blocks):
            z = raw_ref[:, k * Q : (k + 1) * Q] + bias
            small_exp = jnp.exp(-jnp.abs(z))
            step = jnp.maximum(z, 0.0) + jnp.log1p(small_exp)
            gates.append(jnp.where(z >= 0.0, 1.0, small_exp) / (1.0 + small_exp))
            steps.append(step)
            decays.append(-rate * step * LOG2E)
        sums = dn(stack(*decays), upper, HIGHEST)
        logs = [sums[16 * k : 16 * k + 16] for k in range(blocks)]
        ends = [log[:, Q - 1 : Q] for log in logs]
        so_far = jnp.zeros_like(ends[0])
        fill = jnp.zeros((48, Q), f32)
        for k in range(blocks):
            log, step = logs[k], steps[k]
            cols_ref[k * Q : (k + 1) * Q, :] = stack(
                log - jnp.log(step) * LOG2E,
                jnp.exp2(log),
                step * jnp.exp2(ends[k] - log),
                jnp.exp2(log + so_far),
                skip,
                fill,
            ).T
            so_far = so_far + ends[k]
            for r in range(4):
                four = slice(4 * r, 4 * r + 4)
                info_ref[r, :, k * Q : (k + 1) * Q] = stack(
                    log[four], step[four], gates[k][four], rate[four]
                )
            ct_ref[k] = c_ref[k * Q : (k + 1) * Q, :].astype(f32).T.astype(bf16)
            bt_ref[k] = b_ref[k * Q : (k + 1) * Q, :].astype(f32).T.astype(bf16)
        zero_rows = jnp.zeros((4, 128), f32)
        ends_row = []
        for r in range(4):
            last = spread(cols_ref[blocks * Q - 8 : blocks * Q, :], GROW_ALL + 4 * r)[7:8, :]
            ends_row += [last[:, 0:128], last[:, 128:256]]
        for half in range(2):
            tile = stack(*ends_row[4 * half : 4 * half + 4], zero_rows)
            for i in range(16):
                sums_ref[2 * i + half, 32:40, :] = tile

    total = jnp.zeros((128, 256), f32)
    before = None
    for k in range(blocks):
        rows = slice(k * Q, (k + 1) * Q)
        grow = spread(group_cols(cols_ref[rows, :], g), GROW)
        high, low = split(dy_ref[rows, :].astype(f32) * grow)
        high_ref[rows, :] = high
        low_ref[rows, :] = low
        ct = ct_ref[k]
        delta = dn(side(ct, ct), stack(high, low))
        delta_ref[k] = delta
        end = grow[Q - 1 : Q, :]
        total = delta if k == 0 else total + before * delta
        before = end if k == 0 else before * end
    at = pl.ds(pl.multiple_of((g % 2) * 16, 16), 16)
    for i in range(16):
        part = total[8 * i : 8 * i + 8]
        sums_ref[2 * i + g // 2, at, :] = stack(part[:, 0:128], part[:, 128:256])


def carry_kernel(sums_ref, out_ref):
    carried = [jnp.zeros((8, 128), f32) for _ in range(4)]
    for m in reversed(range(sums_ref.shape[0])):
        for r in range(4):
            tile = slice(8 * r, 8 * r + 8)
            out_ref[m, tile, :] = carried[r]
            decay = jnp.broadcast_to(sums_ref[m, 32 + r : 33 + r, :], (8, 128))
            carried[r] = sums_ref[m, tile, :] + decay * carried[r]


def pair_kernel(
    first, x_ref, dy_ref, b_ref, c_ref, cols_ref, info_ref,
    tot_in_ref, adj_ref, tot_ref, rows_ref, gb_ref, gc_ref,
    meet_ref,
):
    step = pl.program_id(0)
    g = step + first
    blocks = x_ref.shape[0] // Q

    @pl.when(step == 0)
    def clear():
        for k in range(blocks):
            rows = slice(k * Q, (k + 1) * Q)
            meet_ref[k] = dt(b_ref[rows, :], c_ref[rows, :])
        if tot_in_ref is None:
            tot_ref[...] = jnp.zeros_like(tot_ref)
        else:
            tot_ref[...] = tot_in_ref[...]

    upper = lax.broadcasted_iota(jnp.int32, (Q, Q), 0) <= lax.broadcasted_iota(
        jnp.int32, (Q, Q), 1
    )
    lane = lax.broadcasted_iota(jnp.int32, (1, 128), 1)
    masks = [
        jnp.where(lane < 64, 1.0, 0.0).astype(bf16),
        jnp.where(lane < 64, 0.0, 1.0).astype(bf16),
    ]

    def one(k):
        rows = pl.ds(pl.multiple_of(k * Q, Q), Q)
        cols = group_cols(cols_ref[rows, :], g)
        meet = meet_ref[k]
        total = tot_ref[k]
        in_rows = []
        for j in range(2):
            lanes = slice(128 * j, 128 * j + 128)
            x_pair, dy_pair = x_ref[rows, lanes], dy_ref[rows, lanes]
            dots = dt(stack(x_pair * masks[0], x_pair * masks[1]), dy_pair)
            weights, values = [], []
            for i in range(2):
                h = 2 * j + i
                gap = info_ref[0, h : h + 1, rows] - jnp.broadcast_to(
                    cols[:, LOGCOL + h : LOGCOL + h + 1], (Q, Q)
                )
                decay = jnp.exp2(jnp.where(upper, gap, -1e30))
                pair = dots[Q * i : Q * i + Q] * decay
                total = total + pair
                in_rows.append(jnp.sum(pair * meet, axis=0, keepdims=True))
                weights += list(split(decay * meet))
                values += [dy_pair * masks[i]] * 2
            adj_ref[rows, lanes] = dn(side(*weights), stack(*values))
        tot_ref[k] = total
        rows_ref[0, 0:4, rows] = stack(*in_rows)

    def some(i, unused):
        for k in range(PAIR_UNROLL):
            one(i * PAIR_UNROLL + k)
        return unused

    lax.fori_loop(0, blocks // PAIR_UNROLL, some, 0)
    if gb_ref is None:
        return

    @pl.when(step == pl.num_programs(0) - 1)
    def finish():
        for k in range(blocks):
            rows = slice(k * Q, (k + 1) * Q)
            total = tot_ref[k]
            high, low = split(total)
            c = c_ref[rows, :]
            gb_ref[rows, :] = dn(side(high, low), stack(c, c))
            high, low = split(total.T)
            b = b_ref[rows, :]
            gc_ref[rows, :] = dn(side(high, low), stack(b, b))


PAIR_UNROLL = 2
LEFT = 3


def three(rows_high, rows_low, high, low):
    both = dt(rows_high, stack(high, low))
    return both[:, 0:128] + both[:, 128:256] + dt(rows_low, high)


def forward_kernel(
    x_ref, high_ref, low_ref, c_ref, bt_ref, cols_ref, start_ref, gc_in_ref,
    gc_ref, rows_ref, end_ref, xhigh_ref, xlow_ref,
    hold_ref,
):
    g = pl.program_id(0)
    blocks = x_ref.shape[0] // Q

    @pl.when(g == 0)
    def copy():
        gc_ref[...] = gc_in_ref[...]

    for h in range(4):
        for q in range(4):
            at = 16 * (h % 2)
            hold_ref[64 * h + 16 * q : 64 * h + 16 * q + 16, :] = start_ref[q, h // 2, at : at + 16, :]
    state = hold_ref[...].T
    for k in range(blocks):
        rows = slice(k * Q, (k + 1) * Q)
        cols = group_cols(cols_ref[rows, :], g)
        x_high, x_low = split(x_ref[rows, :].astype(f32) * spread(cols, SHRINK))
        xhigh_ref[rows, :] = x_high
        xlow_ref[rows, :] = x_low
        bt = bt_ref[k]
        delta = dn(side(bt, bt), stack(x_high, x_low))
        decay = spread(cols[Q - 8 : Q, :], GROW)[7:8, :]
        s_high, s_low = split(state)
        c = c_ref[rows, :]
        from_state = dn(side(c, c), stack(s_high, s_low))
        dy_high, dy_low = high_ref[rows, :], low_ref[rows, :]
        rows_ref[0, 0:4, rows] = head_sums((dy_high.astype(f32) + dy_low.astype(f32)) * from_state)
        gc_ref[rows, :] += three(dy_high, dy_low, s_high, s_low)
        state = decay * state + delta
    end_ref[...] = state


def backward_kernel(
    x_ref, dy_ref, xhigh_ref, xlow_ref, b_ref, cols_ref, info_ref, delta_ref, left_ref, right_ref, gb_in_ref,
    left_rows_ref, right_rows_ref, rows_ref, end_ref, in_ref,
    gx_ref, gb_ref, raw_ref,
    out_ref, grad_ref,
):
    g = pl.program_id(0)
    blocks = x_ref.shape[0] // Q

    @pl.when(g == 0)
    def copy():
        gb_ref[...] = gb_in_ref[...]

    skip = spread(group_cols(cols_ref[0:8, :], g), SKIP)[0:1, :]
    adjoint = side(*[in_ref[:, 0, 8 * r : 8 * r + 8, :].reshape(128, 128) for r in range(2)])
    meeting = jnp.sum(adjoint * end_ref[...], axis=0, keepdims=True)
    row = lax.broadcasted_iota(jnp.int32, (8, 256), 0)
    lane = lax.broadcasted_iota(jnp.int32, (8, 256), 1)
    through = jnp.sum(jnp.where(row == lane // 64, meeting, 0.0), axis=1, keepdims=True)[0:4]
    for k in reversed(range(blocks)):
        rows = slice(k * Q, (k + 1) * Q)
        cols = group_cols(cols_ref[rows, :], g)
        decay = spread(cols[Q - 8 : Q, :], GROW)[7:8, :]
        g_high, g_low = split(adjoint)
        b = b_ref[rows, :]
        adj = jnp.where(g < LEFT, left_ref[rows, :], right_ref[rows, :]) + spread(cols, SHRINK) * dn(side(b, b), stack(g_high, g_low))
        gx_ref[rows, :] = (adj + skip * dy_ref[rows, :].astype(f32)).astype(bf16)
        out_ref[:, rows] = head_sums(x_ref[rows, :].astype(f32) * adj)
        gb_ref[rows, :] += three(xhigh_ref[rows, :], xlow_ref[rows, :], g_high, g_low)
        adjoint = decay * adjoint + delta_ref[k]
    after = jnp.where(
        lax.broadcasted_iota(jnp.int32, (Q, Q), 0) >= lax.broadcasted_iota(jnp.int32, (Q, Q), 1),
        1.0, 0.0,
    )
    parts = []
    for k in range(blocks):
        rows = slice(k * Q, (k + 1) * Q)
        parts.append(
            jnp.where(g < LEFT, left_rows_ref[0, 0:4, rows], right_rows_ref[0, 0:4, rows])
            + rows_ref[0, 0:4, rows] - out_ref[:, rows]
        )
    sums = dn(stack(*parts), after, HIGHEST)
    later = through
    for k in reversed(range(blocks)):
        rows = slice(k * Q, (k + 1) * Q)
        here = sums[4 * k : 4 * k + 4]
        step, gate, rate = (info_ref[0, 4 * r : 4 * r + 4, rows] for r in (1, 2, 3))
        grad_ref[g, :, rows] = gate * (out_ref[:, rows] / step - rate * (here + later))
        later = later + here[:, 0:1]

    @pl.when(g == pl.num_programs(0) - 1)
    def finish():
        for r in range(4):
            raw_ref[4 * r : 4 * r + 4, :] = grad_ref[r]


def whole(shape):
    zeros = (0,) * len(shape)
    return pl.BlockSpec(tuple(shape), lambda g, zeros=zeros: zeros)


def on_device(
    inputs, out_grad, b_proj, c_proj, step_raw, log_rate, step_bias, skip_gain,
    saved_states, segment_slot,
):
    tok = inputs.shape[0]
    blocks = tok // Q
    segs = saved_states.shape[0]
    arbitrary = pltpu.CompilerParams(dimension_semantics=("arbitrary",))

    def shape(*dims, dtype=f32):
        return jax.ShapeDtypeStruct(dims, dtype)

    def cost(flops, bytes_accessed):
        return pl.CostEstimate(
            flops=flops, transcendentals=0, bytes_accessed=bytes_accessed
        )

    quarter = pl.BlockSpec((tok, 256), lambda g: (0, g))
    narrow = whole((tok, 128))
    rows8 = pl.BlockSpec((1, 8, tok), lambda g: (g, 0, 0))
    info_spec = pl.BlockSpec((1, 16, tok), lambda g: (g, 0, 0))
    turn = whole((blocks, 128, Q))
    states = pl.BlockSpec((blocks, 128, 256), lambda g: (0, 0, g))
    state = pl.BlockSpec((128, 256), lambda g: (0, g))
    params = jnp.pad(jnp.stack([log_rate, step_bias, skip_gain]), ((0, 5), (0, 112)))

    sums, cols, info, bt, dy_high, dy_low, deltas = pl.pallas_call(
        first_kernel,
        grid=(4,),
        in_specs=[
            pl.BlockSpec(memory_space=pltpu.SMEM), whole((16, tok)), whole((8, 128)), quarter,
            narrow, narrow, whole((segs, 32, 128)),
        ],
        out_specs=[
            whole((segs, 72, 128)), narrow, whole((4, 16, tok)), turn, quarter, quarter, states,
        ],
        out_shape=(
            shape(segs, 72, 128), shape(tok, 128), shape(4, 16, tok),
            shape(blocks, 128, Q, dtype=bf16), shape(tok, 1024, dtype=bf16),
            shape(tok, 1024, dtype=bf16), shape(blocks, 128, 1024),
        ),
        scratch_shapes=[pltpu.VMEM((128, 128), f32), pltpu.VMEM((blocks, 128, Q), bf16)],
        compiler_params=arbitrary,
        cost_estimate=cost(10**9, 10**7),
        name="first",
    )(
        segment_slot, step_raw.T, params, out_grad, b_proj, c_proj,
        saved_states.reshape(segs, 32, 128),
    )
    sums = lax.all_to_all(sums, "seq", split_axis=0, concat_axis=0, tiled=True)

    def pairs(begin, steps, tot):
        last = tot is not None
        shifted = pl.BlockSpec((tok, 256), lambda g: (0, g + begin))
        info_part = pl.BlockSpec((1, 16, tok), lambda g: (g + begin, 0, 0))
        square = whole((blocks, Q, Q))

        def kernel(*refs):
            ins, outs = list(refs[: 6 + last]), list(refs[6 + last :])
            ins += [] if last else [None]
            outs = outs if last else outs[:3] + [None, None] + outs[3:]
            pair_kernel(begin, *ins, *outs)

        return pl.pallas_call(
            kernel,
            grid=(steps,),
            in_specs=[shifted, shifted, narrow, narrow, narrow, info_part] + [square] * last,
            out_specs=[quarter, square, rows8] + [narrow, narrow] * last,
            out_shape=[
                shape(tok, 256 * steps), shape(blocks, Q, Q), shape(steps, 8, tok)
            ] + [shape(tok, 128)] * (2 * last),
            scratch_shapes=[pltpu.VMEM((blocks, Q, Q), f32)],
            compiler_params=arbitrary,
            cost_estimate=cost(5 * 10**9 * steps, 10**6 * steps),
            name="pairs",
        )(inputs, out_grad, b_proj, c_proj, cols, info, *([tot] * last))

    adj_left, tot, rows_left = pairs(0, LEFT, None)
    sums, rows_left = lax.optimization_barrier((sums, rows_left))
    start = lax.all_to_all(
        sums[:, 40:72].reshape(4, segs // 4, 32, 128),
        "head", split_axis=0, concat_axis=0, tiled=True,
    )
    carried = pl.pallas_call(
        carry_kernel,
        grid=(1,),
        in_specs=[whole((segs, 40, 128))],
        out_specs=whole((segs, 32, 128)),
        out_shape=shape(segs, 32, 128),
        compiler_params=pltpu.CompilerParams(vmem_limit_bytes=8 * 2**20),
        cost_estimate=cost(10**6, 10**6),
        name="carry",
    )(sums)
    carried, tot = lax.optimization_barrier((carried, tot))
    adj_right, tot, rows_right, gb, gc = pairs(LEFT, 4 - LEFT, tot)
    carried, rows_right = lax.optimization_barrier((carried, rows_right))
    incoming = lax.all_to_all(carried, "seq", split_axis=0, concat_axis=0, tiled=True)
    gc, rows, end, x_high, x_low = pl.pallas_call(
        forward_kernel,
        grid=(4,),
        in_specs=[
            quarter, quarter, quarter, narrow, turn, narrow,
            pl.BlockSpec((4, 2, 32, 128), lambda g: (0, g, 0, 0)), narrow,
        ],
        out_specs=[narrow, rows8, state, quarter, quarter],
        out_shape=(
            shape(tok, 128), shape(4, 8, tok), shape(128, 1024),
            shape(tok, 1024, dtype=bf16), shape(tok, 1024, dtype=bf16),
        ),
        scratch_shapes=[pltpu.VMEM((256, 128), f32)],
        compiler_params=arbitrary,
        cost_estimate=cost(3 * 10**9, 10**7),
        name="forward",
    )(inputs, dy_high, dy_low, c_proj, bt, cols, start, gc)
    gc = lax.all_to_all(
        gc.reshape(4, tok // 4, 128), "head", split_axis=0, concat_axis=0, tiled=True
    ).sum(axis=0)
    grad_inputs, gb, grad_step_raw = pl.pallas_call(
        backward_kernel,
        grid=(4,),
        in_specs=[
            quarter, quarter, quarter, quarter, narrow, narrow, info_spec, states,
            pl.BlockSpec((tok, 256), lambda g: (0, jnp.minimum(g, LEFT - 1))),
            pl.BlockSpec((tok, 256), lambda g: (0, jnp.maximum(g, LEFT) - LEFT)),
            narrow,
            pl.BlockSpec((1, 8, tok), lambda g: (jnp.minimum(g, LEFT - 1), 0, 0)),
            pl.BlockSpec((1, 8, tok), lambda g: (jnp.maximum(g, LEFT) - LEFT, 0, 0)),
            rows8, state,
            pl.BlockSpec((16, 1, 16, 128), lambda g: (0, g // 2, g % 2, 0)),
        ],
        out_specs=[quarter, narrow, whole((16, tok))],
        out_shape=(shape(tok, 1024, dtype=bf16), shape(tok, 128), shape(16, tok)),
        scratch_shapes=[pltpu.VMEM((4, tok), f32), pltpu.VMEM((4, 4, tok), f32)],
        compiler_params=arbitrary,
        cost_estimate=cost(3 * 10**9, 10**7),
        name="backward",
    )(
        inputs, out_grad, x_high, x_low, b_proj, cols, info, deltas, adj_left, adj_right,
        gb, rows_left, rows_right, rows,
        end, incoming.reshape(16, 2, 32, 128),
    )
    gb = lax.all_to_all(
        gb.reshape(4, tok // 4, 128), "head", split_axis=0, concat_axis=0, tiled=True
    ).sum(axis=0)
    return grad_inputs, grad_step_raw.T, gb, gc


def solution(mesh):
    return jax.shard_map(
        on_device,
        mesh=mesh,
        in_specs=(
            P("seq", "head"),
            P("seq", "head"),
            P("seq", None),
            P("seq", None),
            P("seq", "head"),
            P("head"),
            P("head"),
            P("head"),
            P(None, "seq", "head", None),
            P(),
        ),
        out_specs=(P("seq", "head"), P("seq", "head"), P(("seq", "head"), None), P(("seq", "head"), None)),
        check_vma=False,
    )
```

```python
import jax
import jax.numpy as jnp
from jax import lax
from jax.experimental import pallas as pl
from jax.experimental.pallas import tpu as pltpu
from jax.sharding import PartitionSpec as P

f32 = jnp.float32
bf16 = jnp.bfloat16
Q = 128
LOG2E = 1.4426950408889634
HIGHEST = lax.Precision.HIGHEST


def dn(a, b, precision=None):
    return lax.dot_general(
        a, b, (((1,), (0,)), ((), ())), precision=precision, preferred_element_type=f32
    )


def dt(a, b, precision=None):
    return lax.dot_general(
        a, b, (((1,), (1,)), ((), ())), precision=precision, preferred_element_type=f32
    )


def split(value):
    high = value.astype(bf16)
    low = (value - high.astype(f32)).astype(bf16)
    return high, low


def side(*parts):
    return jnp.concatenate(parts, axis=1)


def stack(*parts):
    return jnp.concatenate(parts, axis=0)


def spread(cols, base):
    rows = cols.shape[0]
    first = lax.broadcasted_iota(jnp.int32, (rows, 128), 1) < 64
    parts = []
    for j in range(2):
        left, right = (
            jnp.broadcast_to(cols[:, k : k + 1], (rows, 128))
            for k in (base + 2 * j, base + 2 * j + 1)
        )
        parts.append(jnp.where(first, left, right))
    return side(*parts)


def group_cols(cols, group):
    return pltpu.roll(cols, (128 - 4 * group) % 128, 1)


def head_sums(product):
    rows = []
    for j in range(2):
        turned = product[:, 128 * j : 128 * j + 128].T
        for i in range(2):
            part = turned[64 * i : 64 * i + 64]
            eight = part[0:8]
            for r in range(1, 8):
                eight = eight + part[8 * r : 8 * r + 8]
            rows.append(jnp.sum(eight, axis=0, keepdims=True))
    return stack(*rows)


GROW, SHRINK = 0, 32
LOGCOL, GROW_ALL, SKIP = (16 * q for q in range(3))


def repeater(base, group):
    row = lax.broadcasted_iota(jnp.int32, (128, 256), 0) - (base + 4 * group)
    head = lax.broadcasted_iota(jnp.int32, (128, 256), 1) // 64
    return jnp.where((row == head) | (row == head + 16), 1.0, 0.0).astype(bf16)


def first_kernel(
    slot_ref, raw_ref, rate_ref, bias_ref, skip_ref, dy_ref, b_ref, c_ref, saved_ref,
    sums_ref, cols_ref, scales_ref, info_ref, bt_ref, delta_ref,
    pad_ref, ct_ref,
):
    g = pl.program_id(0)
    blocks = dy_ref.shape[0] // Q

    @pl.when(g == 0)
    def prepare():
        for k in range(saved_ref.shape[0]):
            sums_ref[slot_ref[k], 40:72, :] = saved_ref[k]
        pad_ref[0:8, 0:16] = jnp.broadcast_to(jnp.exp(rate_ref[...]), (8, 16))
        pad_ref[8:16, 0:16] = jnp.broadcast_to(bias_ref[...], (8, 16))
        pad_ref[16:24, 0:16] = jnp.broadcast_to(skip_ref[...], (8, 16))
        small = pad_ref[...].T
        rate, bias, skip = (
            jnp.broadcast_to(small[0:16, k : k + 1], (16, Q)) for k in (0, 8, 16)
        )
        row = lax.broadcasted_iota(jnp.int32, (Q, Q), 0)
        lane = lax.broadcasted_iota(jnp.int32, (Q, Q), 1)
        upper = jnp.where(row <= lane, 1.0, 0.0)
        steps, gates, decays = [], [], []
        for k in range(blocks):
            z = raw_ref[:, k * Q : (k + 1) * Q] + bias
            small_exp = jnp.exp(-jnp.abs(z))
            step = jnp.maximum(z, 0.0) + jnp.log1p(small_exp)
            gates.append(jnp.where(z >= 0.0, 1.0, small_exp) / (1.0 + small_exp))
            steps.append(step)
            decays.append(-rate * step * LOG2E)
        sums = dn(stack(*decays), upper, HIGHEST)
        logs = [sums[16 * k : 16 * k + 16] for k in range(blocks)]
        ends = [log[:, Q - 1 : Q] for log in logs]
        so_far = jnp.zeros_like(ends[0])
        fill = jnp.zeros((80, Q), f32)
        fill_scales = jnp.zeros((64, Q), f32)
        for k in range(blocks):
            log, step = logs[k], steps[k]
            cols_ref[k * Q : (k + 1) * Q, :] = stack(
                log - jnp.log(step) * LOG2E,
                jnp.exp2(log + so_far),
                skip,
                fill,
            ).T
            grow, shrink = jnp.exp2(log), step * jnp.exp2(ends[k] - log)
            grow_high, shrink_high = (
                part.astype(bf16).astype(f32) for part in (grow, shrink)
            )
            scales_ref[k * Q : (k + 1) * Q, :] = stack(
                grow_high, grow - grow_high, shrink_high, shrink - shrink_high, fill_scales
            ).T.astype(bf16)
            so_far = so_far + ends[k]
            for r in range(4):
                four = slice(4 * r, 4 * r + 4)
                info_ref[r, :, k * Q : (k + 1) * Q] = stack(
                    log[four], step[four], gates[k][four], rate[four]
                )
            ct_ref[k] = c_ref[k * Q : (k + 1) * Q, :].astype(f32).T.astype(bf16)
            bt_ref[k] = b_ref[k * Q : (k + 1) * Q, :].astype(f32).T.astype(bf16)
        zero_rows = jnp.zeros((4, 128), f32)
        ends_row = []
        for r in range(4):
            last = spread(cols_ref[blocks * Q - 8 : blocks * Q, :], GROW_ALL + 4 * r)[7:8, :]
            ends_row += [last[:, 0:128], last[:, 128:256]]
        for half in range(2):
            tile = stack(*ends_row[4 * half : 4 * half + 4], zero_rows)
            for i in range(16):
                sums_ref[2 * i + half, 32:40, :] = tile

    total = jnp.zeros((128, 256), f32)
    before = None
    grow_to = repeater(GROW, g)
    for k in range(blocks):
        rows = slice(k * Q, (k + 1) * Q)
        grow = dn(scales_ref[rows, :], grow_to)
        high, low = split(dy_ref[rows, :].astype(f32) * grow)
        ct = ct_ref[k]
        delta = dn(side(ct, ct), stack(high, low))
        delta_ref[0, k] = delta
        end = grow[Q - 1 : Q, :]
        total = delta if k == 0 else total + before * delta
        before = end if k == 0 else before * end
    at = pl.ds(pl.multiple_of((g % 2) * 16, 16), 16)
    for i in range(16):
        part = total[8 * i : 8 * i + 8]
        sums_ref[2 * i + g // 2, at, :] = stack(part[:, 0:128], part[:, 128:256])


def carry_kernel(sums_ref, out_ref):
    carried = [jnp.zeros((8, 128), f32) for _ in range(4)]
    for m in reversed(range(sums_ref.shape[0])):
        for r in range(4):
            tile = slice(8 * r, 8 * r + 8)
            out_ref[m, tile, :] = carried[r]
            decay = jnp.broadcast_to(sums_ref[m, 32 + r : 33 + r, :], (8, 128))
            carried[r] = sums_ref[m, tile, :] + decay * carried[r]


def pair_kernel(
    first, x_ref, dy_ref, b_ref, c_ref, cols_ref, info_ref,
    tot_in_ref, adj_ref, tot_ref, rows_ref, gb_ref, gc_ref,
    meet_ref,
):
    step = pl.program_id(0)
    g = step + first
    blocks = x_ref.shape[0] // Q

    @pl.when(step == 0)
    def clear():
        for k in range(blocks):
            rows = slice(k * Q, (k + 1) * Q)
            meet_ref[k] = dt(b_ref[rows, :], c_ref[rows, :])
        if tot_in_ref is None:
            tot_ref[...] = jnp.zeros_like(tot_ref)
        else:
            tot_ref[...] = tot_in_ref[...]

    upper = lax.broadcasted_iota(jnp.int32, (Q, Q), 0) <= lax.broadcasted_iota(
        jnp.int32, (Q, Q), 1
    )
    lane = lax.broadcasted_iota(jnp.int32, (1, 128), 1)
    masks = [
        jnp.where(lane < 64, 1.0, 0.0).astype(bf16),
        jnp.where(lane < 64, 0.0, 1.0).astype(bf16),
    ]

    def one(k):
        rows = pl.ds(pl.multiple_of(k * Q, Q), Q)
        cols = group_cols(cols_ref[rows, :], g)
        meet = meet_ref[k]
        total = tot_ref[k]
        in_rows = []
        for j in range(2):
            lanes = slice(128 * j, 128 * j + 128)
            x_pair, dy_pair = x_ref[rows, lanes], dy_ref[rows, lanes]
            dots = dt(stack(x_pair * masks[0], x_pair * masks[1]), dy_pair)
            weights, values = [], []
            for i in range(2):
                h = 2 * j + i
                gap = info_ref[0, h : h + 1, rows] - jnp.broadcast_to(
                    cols[:, LOGCOL + h : LOGCOL + h + 1], (Q, Q)
                )
                decay = jnp.exp2(jnp.where(upper, gap, -1e30))
                pair = dots[Q * i : Q * i + Q] * decay
                total = total + pair
                in_rows.append(jnp.sum(pair * meet, axis=0, keepdims=True))
                weights += list(split(decay * meet))
                values += [dy_pair * masks[i]] * 2
            adj_ref[0, rows, lanes] = dn(side(*weights), stack(*values))
        tot_ref[k] = total
        rows_ref[0, 0:4, rows] = stack(*in_rows)

    def some(i, unused):
        for k in range(PAIR_UNROLL):
            one(i * PAIR_UNROLL + k)
        return unused

    lax.fori_loop(0, blocks // PAIR_UNROLL, some, 0)
    if gb_ref is None:
        return

    @pl.when(step == pl.num_programs(0) - 1)
    def finish():
        for k in range(blocks):
            rows = slice(k * Q, (k + 1) * Q)
            total = tot_ref[k]
            high, low = split(total)
            c = c_ref[rows, :]
            gb_ref[rows, :] = dn(side(high, low), stack(c, c))
            high, low = split(total.T)
            b = b_ref[rows, :]
            gc_ref[rows, :] = dn(side(high, low), stack(b, b))


PAIR_UNROLL = 8
LEFT = 3


def three(rows_high, rows_low, high, low):
    both = dt(rows_high, stack(high, low))
    return both[:, 0:128] + both[:, 128:256] + dt(rows_low, high)


def forward_kernel(
    x_ref, dy_ref, c_ref, bt_ref, scales_ref, start_ref, gc_in_ref,
    gc_ref, rows_ref, end_ref,
    hold_ref, grow_ref, shrink_ref,
):
    g = pl.program_id(0)
    blocks = x_ref.shape[0] // Q

    @pl.when(g == 0)
    def copy():
        gc_ref[...] = gc_in_ref[...]

    for h in range(4):
        for q in range(4):
            at = 16 * (h % 2)
            hold_ref[64 * h + 16 * q : 64 * h + 16 * q + 16, :] = start_ref[q, h // 2, at : at + 16, :]
    state = hold_ref[...].T
    grow_ref[...] = dn(scales_ref[...], repeater(GROW, g))
    shrink_ref[...] = dn(scales_ref[...], repeater(SHRINK, g))
    for k in range(blocks):
        rows = slice(k * Q, (k + 1) * Q)
        grow = grow_ref[rows, :]
        x_high, x_low = split(x_ref[rows, :].astype(f32) * shrink_ref[rows, :])
        bt = bt_ref[k]
        delta = dn(side(bt, bt), stack(x_high, x_low))
        s_high, s_low = split(state)
        c = c_ref[rows, :]
        from_state = dn(side(c, c), stack(s_high, s_low))
        dy_grown = dy_ref[rows, :].astype(f32) * grow
        dy_high, dy_low = split(dy_grown)
        rows_ref[0, 0:4, rows] = head_sums(dy_grown * from_state)
        gc_ref[rows, :] += three(dy_high, dy_low, s_high, s_low)
        state = grow[Q - 1 : Q, :] * state + delta
    end_ref[0] = state


def backward_kernel(
    x_ref, dy_ref, b_ref, cols_ref, scales_ref, info_ref, delta_ref, adj_ref, gb_in_ref,
    pair_rows_ref, rows_ref, end_ref, in_ref,
    gx_ref, gb_ref, raw_ref,
    keep_ref, through_ref, shrink_ref,
):
    g = pl.program_id(0)
    blocks = x_ref.shape[0] // Q

    @pl.when(g == 0)
    def copy():
        gb_ref[...] = gb_in_ref[...]

    skip = spread(group_cols(cols_ref[0:8, :], g), SKIP)[0:1, :]
    adjoint = side(*[in_ref[:, 0, 8 * r : 8 * r + 8, :].reshape(128, 128) for r in range(2)])
    meeting = jnp.sum(adjoint * end_ref[0], axis=0, keepdims=True)
    row = lax.broadcasted_iota(jnp.int32, (8, 256), 0)
    lane = lax.broadcasted_iota(jnp.int32, (8, 256), 1)
    through = jnp.sum(jnp.where(row == lane // 64, meeting, 0.0), axis=1, keepdims=True)[0:4]
    shrink_ref[...] = dn(scales_ref[...], repeater(SHRINK, g))
    ends = stack(*[scales_ref[k * Q + Q - 16 : k * Q + Q, :] for k in range(blocks)])
    decays = dn(ends, repeater(GROW, g))
    for k in reversed(range(blocks)):
        rows = slice(k * Q, (k + 1) * Q)
        shrink = shrink_ref[rows, :]
        x_full = x_ref[rows, :].astype(f32)
        x_high, x_low = split(x_full * shrink)
        g_high, g_low = split(adjoint)
        b = b_ref[rows, :]
        adj = adj_ref[0, rows, :] + shrink * dn(
            side(b, b), stack(g_high, g_low)
        )
        gx_ref[rows, :] = (adj + skip * dy_ref[rows, :].astype(f32)).astype(bf16)
        out_rows = head_sums(x_full * adj)
        gb_ref[rows, :] += three(x_high, x_low, g_high, g_low)
        adjoint = decays[16 * k + 15 : 16 * k + 16, :] * adjoint + delta_ref[0, k]
        keep_ref[g, 0:4, rows] = (
            pair_rows_ref[0, 0:4, rows] + rows_ref[0, 0:4, rows] - out_rows
        )
        keep_ref[g, 4:8, rows] = out_rows
    through_ref[g] = jnp.broadcast_to(through, (4, Q))

    @pl.when(g == pl.num_programs(0) - 1)
    def finish():
        after = jnp.where(
            lax.broadcasted_iota(jnp.int32, (Q, Q), 0)
            >= lax.broadcasted_iota(jnp.int32, (Q, Q), 1),
            1.0, 0.0,
        )

        def all_heads(ref, first, rows):
            return stack(*[ref[r, first : first + 4, rows] for r in range(4)])

        parts = [all_heads(keep_ref, 0, slice(k * Q, (k + 1) * Q)) for k in range(blocks)]
        sums = dn(stack(*parts), after, HIGHEST)
        later = stack(*[through_ref[r][:, 0:1] for r in range(4)])
        for k in reversed(range(blocks)):
            rows = slice(k * Q, (k + 1) * Q)
            here = sums[16 * k : 16 * k + 16]
            step, gate, rate = (all_heads(info_ref, 4 * r, rows) for r in (1, 2, 3))
            x_adj = all_heads(keep_ref, 4, rows)
            raw_ref[:, rows] = gate * (x_adj / step - rate * (here + later))
            later = later + here[:, 0:1]


def whole(shape):
    zeros = (0,) * len(shape)
    return pl.BlockSpec(tuple(shape), lambda g, zeros=zeros: zeros)


def on_device(
    inputs, out_grad, b_proj, c_proj, step_raw, log_rate, step_bias, skip_gain,
    saved_states, segment_slot,
):
    tok = inputs.shape[0]
    blocks = tok // Q
    segs = saved_states.shape[0]
    arbitrary = pltpu.CompilerParams(dimension_semantics=("arbitrary",))

    def shape(*dims, dtype=f32):
        return jax.ShapeDtypeStruct(dims, dtype)

    def cost(flops, bytes_accessed):
        return pl.CostEstimate(
            flops=flops, transcendentals=0, bytes_accessed=bytes_accessed
        )

    quarter = pl.BlockSpec((tok, 256), lambda g: (0, g))
    narrow = whole((tok, 128))
    rows8 = pl.BlockSpec((1, 8, tok), lambda g: (g, 0, 0))
    info_spec = pl.BlockSpec((1, 16, tok), lambda g: (g, 0, 0))
    turn = whole((blocks, 128, Q))
    states = pl.BlockSpec((1, blocks, 128, 256), lambda g: (g, 0, 0, 0))
    block = pl.BlockSpec((1, tok, 256), lambda g: (g, 0, 0))
    state = pl.BlockSpec((1, 128, 256), lambda g: (g, 0, 0))
    sums, cols, scales, info, bt, deltas = pl.pallas_call(
        first_kernel,
        grid=(4,),
        in_specs=[
            pl.BlockSpec(memory_space=pltpu.SMEM), whole((16, tok)), whole((1, 16)),
            whole((1, 16)), whole((1, 16)), quarter,
            narrow, narrow, whole((segs, 32, 128)),
        ],
        out_specs=[
            whole((segs, 72, 128)), narrow, narrow, whole((4, 16, tok)), turn, states,
        ],
        out_shape=(
            shape(segs, 72, 128), shape(tok, 128), shape(tok, 128, dtype=bf16),
            shape(4, 16, tok), shape(blocks, 128, Q, dtype=bf16), shape(4, blocks, 128, 256),
        ),
        scratch_shapes=[pltpu.VMEM((128, 128), f32), pltpu.VMEM((blocks, 128, Q), bf16)],
        compiler_params=arbitrary,
        cost_estimate=cost(10**9, 10**7),
        name="first",
    )(
        segment_slot, step_raw.T, log_rate[None], step_bias[None], skip_gain[None], out_grad, b_proj, c_proj,
        saved_states.reshape(segs, 32, 128),
    )
    sums = lax.all_to_all(sums, "seq", split_axis=0, concat_axis=0, tiled=True)

    def pairs(begin, steps, *before):
        last = len(before) > 0
        shifted = pl.BlockSpec((tok, 256), lambda g: (0, g + begin))
        info_part = pl.BlockSpec((1, 16, tok), lambda g: (g + begin, 0, 0))
        square = whole((blocks, Q, Q))
        hbm = pl.BlockSpec(memory_space=pl.ANY)

        def kernel(*refs):
            ins, outs = list(refs[:6]), list(refs[6:])
            if last:
                ins, outs = ins + [outs[0]], outs[3:]
            else:
                ins, outs = ins + [None], outs[:3] + [None, None] + outs[3:]
            pair_kernel(begin, *ins, *outs)

        return pl.pallas_call(
            kernel,
            grid=(steps,),
            in_specs=[shifted, shifted, narrow, narrow, narrow, info_part]
            + [square, hbm, hbm] * last,
            out_specs=[
                pl.BlockSpec((1, tok, 256), lambda g: (g + begin, 0, 0)),
                square,
                pl.BlockSpec((1, 8, tok), lambda g: (g + begin, 0, 0)),
            ]
            + [narrow, narrow] * last,
            out_shape=[shape(4, tok, 256), shape(blocks, Q, Q), shape(4, 8, tok)]
            + [shape(tok, 128)] * (2 * last),
            scratch_shapes=[pltpu.VMEM((blocks, Q, Q), f32)],
            input_output_aliases={7: 0, 8: 2} if last else {},
            compiler_params=arbitrary,
            cost_estimate=cost(5 * 10**9 * steps, 10**6 * steps),
            name="pairs",
        )(inputs, out_grad, b_proj, c_proj, cols, info, *before)

    adj, tot, pair_rows = pairs(0, LEFT)
    sums, tot = lax.optimization_barrier((sums, tot))
    start = lax.all_to_all(
        sums[:, 40:72].reshape(4, segs // 4, 32, 128),
        "head", split_axis=0, concat_axis=0, tiled=True,
    )
    carried = pl.pallas_call(
        carry_kernel,
        grid=(1,),
        in_specs=[whole((segs, 40, 128))],
        out_specs=whole((segs, 32, 128)),
        out_shape=shape(segs, 32, 128),
        compiler_params=pltpu.CompilerParams(vmem_limit_bytes=8 * 2**20),
        cost_estimate=cost(10**6, 10**6),
        name="carry",
    )(sums)
    carried, tot = lax.optimization_barrier((carried, tot))
    adj, tot, pair_rows, gb, gc = pairs(LEFT, 4 - LEFT, tot, adj, pair_rows)
    carried, gb = lax.optimization_barrier((carried, gb))
    incoming = lax.all_to_all(carried, "seq", split_axis=0, concat_axis=0, tiled=True)
    gc, rows, end = pl.pallas_call(
        forward_kernel,
        grid=(4,),
        in_specs=[
            quarter, quarter, narrow, turn, narrow,
            pl.BlockSpec((4, 2, 32, 128), lambda g: (0, g, 0, 0)), narrow,
        ],
        out_specs=[narrow, rows8, state],
        out_shape=(
            shape(tok, 128), shape(4, 8, tok), shape(4, 128, 256),
        ),
        scratch_shapes=[
            pltpu.VMEM((256, 128), f32), pltpu.VMEM((tok, 256), f32), pltpu.VMEM((tok, 256), f32)
        ],
        compiler_params=arbitrary,
        cost_estimate=cost(3 * 10**9, 10**7),
        name="forward",
    )(inputs, out_grad, c_proj, bt, scales, start, gc)
    gc = lax.all_to_all(
        gc.reshape(4, tok // 4, 128), "head", split_axis=0, concat_axis=0, tiled=True
    ).sum(axis=0)
    grad_inputs, gb, grad_step_raw = pl.pallas_call(
        backward_kernel,
        grid=(4,),
        in_specs=[
            quarter, quarter, narrow, narrow, narrow, whole((4, 16, tok)), states,
            block, narrow, rows8,
            rows8, state,
            pl.BlockSpec((16, 1, 16, 128), lambda g: (0, g // 2, g % 2, 0)),
        ],
        out_specs=[quarter, narrow, whole((16, tok))],
        out_shape=(shape(tok, 1024, dtype=bf16), shape(tok, 128), shape(16, tok)),
        scratch_shapes=[
            pltpu.VMEM((4, 8, tok), f32), pltpu.VMEM((4, 4, Q), f32), pltpu.VMEM((tok, 256), f32)
        ],
        compiler_params=arbitrary,
        cost_estimate=cost(3 * 10**9, 10**7),
        name="backward",
    )(
        inputs, out_grad, b_proj, cols, scales, info, deltas, adj, gb, pair_rows, rows,
        end, incoming.reshape(16, 2, 32, 128),
    )
    gb = lax.all_to_all(
        gb.reshape(4, tok // 4, 128), "head", split_axis=0, concat_axis=0, tiled=True
    ).sum(axis=0)
    return grad_inputs, grad_step_raw.T, gb, gc


def solution(mesh):
    return jax.shard_map(
        on_device,
        mesh=mesh,
        in_specs=(
            P("seq", "head"),
            P("seq", "head"),
            P("seq", None),
            P("seq", None),
            P("seq", "head"),
            P("head"),
            P("head"),
            P("head"),
            P(None, "seq", "head", None),
            P(),
        ),
        out_specs=(P("seq", "head"), P("seq", "head"), P(("seq", "head"), None), P(("seq", "head"), None)),
        check_vma=False,
    )
```

```python
import jax
import jax.numpy as jnp
from jax import lax
from jax.experimental import pallas as pl
from jax.experimental.pallas import tpu as pltpu
from jax.sharding import PartitionSpec as P

f32 = jnp.float32
bf16 = jnp.bfloat16
Q = 128
LOG2E = 1.4426950408889634
HIGHEST = lax.Precision.HIGHEST


def dn(a, b, precision=None):
    return lax.dot_general(
        a, b, (((1,), (0,)), ((), ())), precision=precision, preferred_element_type=f32
    )


def dt(a, b, precision=None):
    return lax.dot_general(
        a, b, (((1,), (1,)), ((), ())), precision=precision, preferred_element_type=f32
    )


def split(value):
    high = value.astype(bf16)
    low = (value - high.astype(f32)).astype(bf16)
    return high, low


def side(*parts):
    return jnp.concatenate(parts, axis=1)


def stack(*parts):
    return jnp.concatenate(parts, axis=0)


def spread(cols, base):
    rows = cols.shape[0]
    first = lax.broadcasted_iota(jnp.int32, (rows, 128), 1) < 64
    parts = []
    for j in range(2):
        left, right = (
            jnp.broadcast_to(cols[:, k : k + 1], (rows, 128))
            for k in (base + 2 * j, base + 2 * j + 1)
        )
        parts.append(jnp.where(first, left, right))
    return side(*parts)


def group_cols(cols, group):
    return pltpu.roll(cols, (128 - 4 * group) % 128, 1)


def head_sums(product):
    rows = []
    for j in range(2):
        turned = product[:, 128 * j : 128 * j + 128].T
        for i in range(2):
            part = turned[64 * i : 64 * i + 64]
            eight = part[0:8]
            for r in range(1, 8):
                eight = eight + part[8 * r : 8 * r + 8]
            rows.append(jnp.sum(eight, axis=0, keepdims=True))
    return stack(*rows)


GROW, SHRINK = 0, 32
LOGCOL, GROW_ALL, SKIP = (16 * q for q in range(3))


def repeater(base, group):
    row = lax.broadcasted_iota(jnp.int32, (128, 256), 0) - (base + 4 * group)
    head = lax.broadcasted_iota(jnp.int32, (128, 256), 1) // 64
    return jnp.where((row == head) | (row == head + 16), 1.0, 0.0).astype(bf16)


def first_kernel(
    slot_ref, raw_ref, rate_ref, bias_ref, skip_ref, dy_ref, b_ref, c_ref, saved_ref,
    sums_ref, cols_ref, scales_ref, info_ref, bt_ref, delta_ref,
    pad_ref, ct_ref,
):
    g = pl.program_id(0)
    blocks = dy_ref.shape[0] // Q

    @pl.when(g == 0)
    def prepare():
        for k in range(saved_ref.shape[0]):
            sums_ref[slot_ref[k], 40:72, :] = saved_ref[k]
        pad_ref[0:8, 0:16] = jnp.broadcast_to(jnp.exp(rate_ref[...]), (8, 16))
        pad_ref[8:16, 0:16] = jnp.broadcast_to(bias_ref[...], (8, 16))
        pad_ref[16:24, 0:16] = jnp.broadcast_to(skip_ref[...], (8, 16))
        small = pad_ref[...].T
        rate, bias, skip = (
            jnp.broadcast_to(small[0:16, k : k + 1], (16, Q)) for k in (0, 8, 16)
        )
        row = lax.broadcasted_iota(jnp.int32, (Q, Q), 0)
        lane = lax.broadcasted_iota(jnp.int32, (Q, Q), 1)
        upper = jnp.where(row <= lane, 1.0, 0.0)
        steps, gates, decays = [], [], []
        for k in range(blocks):
            z = raw_ref[:, k * Q : (k + 1) * Q] + bias
            small_exp = jnp.exp(-jnp.abs(z))
            step = jnp.maximum(z, 0.0) + jnp.log1p(small_exp)
            gates.append(jnp.where(z >= 0.0, 1.0, small_exp) / (1.0 + small_exp))
            steps.append(step)
            decays.append(-rate * step * LOG2E)
        sums = dn(stack(*decays), upper, HIGHEST)
        logs = [sums[16 * k : 16 * k + 16] for k in range(blocks)]
        ends = [log[:, Q - 1 : Q] for log in logs]
        so_far = jnp.zeros_like(ends[0])
        fill = jnp.zeros((80, Q), f32)
        fill_scales = jnp.zeros((64, Q), f32)
        for k in range(blocks):
            log, step = logs[k], steps[k]
            cols_ref[k * Q : (k + 1) * Q, :] = stack(
                log - jnp.log(step) * LOG2E,
                jnp.exp2(log + so_far),
                skip,
                fill,
            ).T
            grow, shrink = jnp.exp2(log), step * jnp.exp2(ends[k] - log)
            grow_high, shrink_high = (
                part.astype(bf16).astype(f32) for part in (grow, shrink)
            )
            scales_ref[k * Q : (k + 1) * Q, :] = stack(
                grow_high, grow - grow_high, shrink_high, shrink - shrink_high, fill_scales
            ).T.astype(bf16)
            so_far = so_far + ends[k]
            for r in range(4):
                four = slice(4 * r, 4 * r + 4)
                info_ref[r, :, k * Q : (k + 1) * Q] = stack(
                    log[four], step[four], gates[k][four], rate[four]
                )
            ct_ref[k] = c_ref[k * Q : (k + 1) * Q, :].astype(f32).T.astype(bf16)
            bt_ref[k] = b_ref[k * Q : (k + 1) * Q, :].astype(f32).T.astype(bf16)
        zero_rows = jnp.zeros((4, 128), f32)
        ends_row = []
        for r in range(4):
            last = spread(cols_ref[blocks * Q - 8 : blocks * Q, :], GROW_ALL + 4 * r)[7:8, :]
            ends_row += [last[:, 0:128], last[:, 128:256]]
        for half in range(2):
            tile = stack(*ends_row[4 * half : 4 * half + 4], zero_rows)
            for i in range(16):
                sums_ref[2 * i + half, 32:40, :] = tile

    total = jnp.zeros((128, 256), f32)
    before = None
    grow_to = repeater(GROW, g)
    for k in range(blocks):
        rows = slice(k * Q, (k + 1) * Q)
        grow = dn(scales_ref[rows, :], grow_to)
        high, low = split(dy_ref[rows, :].astype(f32) * grow)
        ct = ct_ref[k]
        delta = dn(side(ct, ct), stack(high, low))
        delta_ref[0, k] = delta
        end = grow[Q - 1 : Q, :]
        total = delta if k == 0 else total + before * delta
        before = end if k == 0 else before * end
    at = pl.ds(pl.multiple_of((g % 2) * 16, 16), 16)
    for i in range(16):
        part = total[8 * i : 8 * i + 8]
        sums_ref[2 * i + g // 2, at, :] = stack(part[:, 0:128], part[:, 128:256])


def carry_kernel(sums_ref, out_ref, *start_refs):
    here = lax.axis_index("head")
    for d in range(4):
        group = lax.rem(here + d, 4)
        start_refs[d][...] = sums_ref[pl.ds(pl.multiple_of(group * 8, 8), 8), 40:72, :]
    carried = [jnp.zeros((8, 128), f32) for _ in range(4)]
    for m in reversed(range(sums_ref.shape[0])):
        for r in range(4):
            tile = slice(8 * r, 8 * r + 8)
            out_ref[m, tile, :] = carried[r]
            decay = jnp.broadcast_to(sums_ref[m, 32 + r : 33 + r, :], (8, 128))
            carried[r] = sums_ref[m, tile, :] + decay * carried[r]


def pair_kernel(
    first, x_ref, dy_ref, b_ref, c_ref, cols_ref, info_ref,
    tot_in_ref, adj_ref, tot_ref, rows_ref, gb_ref, gc_ref,
    meet_ref,
):
    step = pl.program_id(0)
    g = step + first
    blocks = x_ref.shape[0] // Q

    @pl.when(step == 0)
    def clear():
        for k in range(blocks):
            rows = slice(k * Q, (k + 1) * Q)
            meet_ref[k] = dt(b_ref[rows, :], c_ref[rows, :])
        if tot_in_ref is None:
            tot_ref[...] = jnp.zeros_like(tot_ref)
        else:
            tot_ref[...] = tot_in_ref[...]

    upper = lax.broadcasted_iota(jnp.int32, (Q, Q), 0) <= lax.broadcasted_iota(
        jnp.int32, (Q, Q), 1
    )
    lane = lax.broadcasted_iota(jnp.int32, (1, 128), 1)
    masks = [
        jnp.where(lane < 64, 1.0, 0.0).astype(bf16),
        jnp.where(lane < 64, 0.0, 1.0).astype(bf16),
    ]

    def one(k):
        rows = pl.ds(pl.multiple_of(k * Q, Q), Q)
        cols = group_cols(cols_ref[rows, :], g)
        meet = meet_ref[k]
        total = tot_ref[k]
        in_rows = []
        for j in range(2):
            lanes = slice(128 * j, 128 * j + 128)
            x_pair, dy_pair = x_ref[rows, lanes], dy_ref[rows, lanes]
            dots = dt(stack(x_pair * masks[0], x_pair * masks[1]), dy_pair)
            weights, values = [], []
            for i in range(2):
                h = 2 * j + i
                gap = info_ref[0, h : h + 1, rows] - jnp.broadcast_to(
                    cols[:, LOGCOL + h : LOGCOL + h + 1], (Q, Q)
                )
                decay = jnp.exp2(jnp.where(upper, gap, -1e30))
                pair = dots[Q * i : Q * i + Q] * decay
                total = total + pair
                in_rows.append(jnp.sum(pair * meet, axis=0, keepdims=True))
                weights += list(split(decay * meet))
                values += [dy_pair * masks[i]] * 2
            adj_ref[0, rows, lanes] = dn(side(*weights), stack(*values))
        tot_ref[k] = total
        rows_ref[0, 0:4, rows] = stack(*in_rows)

    def some(i, unused):
        for k in range(PAIR_UNROLL):
            one(i * PAIR_UNROLL + k)
        return unused

    lax.fori_loop(0, blocks // PAIR_UNROLL, some, 0)
    if gb_ref is None:
        return

    @pl.when(step == pl.num_programs(0) - 1)
    def finish():
        for k in range(blocks):
            rows = slice(k * Q, (k + 1) * Q)
            total = tot_ref[k]
            high, low = split(total)
            c = c_ref[rows, :]
            gb_ref[rows, :] = dn(side(high, low), stack(c, c))
            high, low = split(total.T)
            b = b_ref[rows, :]
            gc_ref[rows, :] = dn(side(high, low), stack(b, b))


PAIR_UNROLL = 8
LEFT = 3


def three(rows_high, rows_low, high, low):
    both = dt(rows_high, stack(high, low))
    return both[:, 0:128] + both[:, 128:256] + dt(rows_low, high)


def forward_kernel(
    x_ref, dy_ref, c_ref, bt_ref, scales_ref, start0_ref, start1_ref, start2_ref, start3_ref, gc_in_ref,
    gc_ref, rows_ref, end_ref,
    hold_ref, grow_ref, shrink_ref,
):
    g = pl.program_id(0)
    blocks = x_ref.shape[0] // Q

    @pl.when(g == 0)
    def copy():
        gc_ref[...] = gc_in_ref[...]

    here = lax.axis_index("head")
    for d, start_ref in enumerate((start0_ref, start1_ref, start2_ref, start3_ref)):
        part = lax.rem(here + 4 - d, 4)
        for h in range(4):
            at = 16 * (h % 2)
            to = pl.ds(pl.multiple_of(64 * h + 16 * part, 16), 16)
            hold_ref[to, :] = start_ref[h // 2, at : at + 16, :]
    state = hold_ref[...].T
    grow_ref[...] = dn(scales_ref[...], repeater(GROW, g))
    shrink_ref[...] = dn(scales_ref[...], repeater(SHRINK, g))
    for k in range(blocks):
        rows = slice(k * Q, (k + 1) * Q)
        grow = grow_ref[rows, :]
        x_high, x_low = split(x_ref[rows, :].astype(f32) * shrink_ref[rows, :])
        bt = bt_ref[k]
        delta = dn(side(bt, bt), stack(x_high, x_low))
        s_high, s_low = split(state)
        c = c_ref[rows, :]
        from_state = dn(side(c, c), stack(s_high, s_low))
        dy_grown = dy_ref[rows, :].astype(f32) * grow
        dy_high, dy_low = split(dy_grown)
        rows_ref[0, 0:4, rows] = head_sums(dy_grown * from_state)
        gc_ref[rows, :] += three(dy_high, dy_low, s_high, s_low)
        state = grow[Q - 1 : Q, :] * state + delta
    end_ref[0] = state


def backward_kernel(
    x_ref, dy_ref, b_ref, cols_ref, scales_ref, info_ref, delta_ref, adj_ref, gb_in_ref,
    pair_rows_ref, rows_ref, end_ref, in_ref,
    gx_ref, raw_ref, gb0_ref, gb1_ref, gb2_ref, gb3_ref,
    gb_ref, keep_ref, through_ref, shrink_ref,
):
    g = pl.program_id(0)
    blocks = x_ref.shape[0] // Q

    @pl.when(g == 0)
    def copy():
        gb_ref[...] = gb_in_ref[...]

    skip = spread(group_cols(cols_ref[0:8, :], g), SKIP)[0:1, :]
    adjoint = side(*[in_ref[:, 0, 8 * r : 8 * r + 8, :].reshape(128, 128) for r in range(2)])
    meeting = jnp.sum(adjoint * end_ref[0], axis=0, keepdims=True)
    row = lax.broadcasted_iota(jnp.int32, (8, 256), 0)
    lane = lax.broadcasted_iota(jnp.int32, (8, 256), 1)
    through = jnp.sum(jnp.where(row == lane // 64, meeting, 0.0), axis=1, keepdims=True)[0:4]
    shrink_ref[...] = dn(scales_ref[...], repeater(SHRINK, g))
    ends = stack(*[scales_ref[k * Q + Q - 16 : k * Q + Q, :] for k in range(blocks)])
    decays = dn(ends, repeater(GROW, g))
    for k in reversed(range(blocks)):
        rows = slice(k * Q, (k + 1) * Q)
        shrink = shrink_ref[rows, :]
        x_full = x_ref[rows, :].astype(f32)
        x_high, x_low = split(x_full * shrink)
        g_high, g_low = split(adjoint)
        b = b_ref[rows, :]
        adj = adj_ref[0, rows, :] + shrink * dn(
            side(b, b), stack(g_high, g_low)
        )
        gx_ref[rows, :] = (adj + skip * dy_ref[rows, :].astype(f32)).astype(bf16)
        out_rows = head_sums(x_full * adj)
        gb_ref[rows, :] += three(x_high, x_low, g_high, g_low)
        adjoint = decays[16 * k + 15 : 16 * k + 16, :] * adjoint + delta_ref[0, k]
        keep_ref[g, 0:4, rows] = (
            pair_rows_ref[0, 0:4, rows] + rows_ref[0, 0:4, rows] - out_rows
        )
        keep_ref[g, 4:8, rows] = out_rows
    through_ref[g] = jnp.broadcast_to(through, (4, Q))

    @pl.when(g == pl.num_programs(0) - 1)
    def finish():
        here = lax.axis_index("head")
        for d, part_ref in enumerate((gb0_ref, gb1_ref, gb2_ref, gb3_ref)):
            size = part_ref.shape[0]
            at = lax.rem(here + d, 4) * size
            part_ref[...] = gb_ref[pl.ds(pl.multiple_of(at, size), size), :]
        after = jnp.where(
            lax.broadcasted_iota(jnp.int32, (Q, Q), 0)
            >= lax.broadcasted_iota(jnp.int32, (Q, Q), 1),
            1.0, 0.0,
        )

        def all_heads(ref, first, rows):
            return stack(*[ref[r, first : first + 4, rows] for r in range(4)])

        parts = [all_heads(keep_ref, 0, slice(k * Q, (k + 1) * Q)) for k in range(blocks)]
        sums = dn(stack(*parts), after, HIGHEST)
        later = stack(*[through_ref[r][:, 0:1] for r in range(4)])
        for k in reversed(range(blocks)):
            rows = slice(k * Q, (k + 1) * Q)
            here = sums[16 * k : 16 * k + 16]
            step, gate, rate = (all_heads(info_ref, 4 * r, rows) for r in (1, 2, 3))
            x_adj = all_heads(keep_ref, 4, rows)
            raw_ref[:, rows] = gate * (x_adj / step - rate * (here + later))
            later = later + here[:, 0:1]


def whole(shape):
    zeros = (0,) * len(shape)
    return pl.BlockSpec(tuple(shape), lambda g, zeros=zeros: zeros)


def around(array, distance):
    if distance == 0:
        return array
    heads = lax.axis_size("head")
    return lax.ppermute(array, "head", [(i, (i + distance) % heads) for i in range(heads)])


def on_device(
    inputs, out_grad, b_proj, c_proj, step_raw, log_rate, step_bias, skip_gain,
    saved_states, segment_slot,
):
    tok = inputs.shape[0]
    blocks = tok // Q
    segs = saved_states.shape[0]
    arbitrary = pltpu.CompilerParams(dimension_semantics=("arbitrary",))

    def shape(*dims, dtype=f32):
        return jax.ShapeDtypeStruct(dims, dtype)

    def cost(flops, bytes_accessed):
        return pl.CostEstimate(
            flops=flops, transcendentals=0, bytes_accessed=bytes_accessed
        )

    quarter = pl.BlockSpec((tok, 256), lambda g: (0, g))
    narrow = whole((tok, 128))
    rows8 = pl.BlockSpec((1, 8, tok), lambda g: (g, 0, 0))
    info_spec = pl.BlockSpec((1, 16, tok), lambda g: (g, 0, 0))
    turn = whole((blocks, 128, Q))
    states = pl.BlockSpec((1, blocks, 128, 256), lambda g: (g, 0, 0, 0))
    block = pl.BlockSpec((1, tok, 256), lambda g: (g, 0, 0))
    state = pl.BlockSpec((1, 128, 256), lambda g: (g, 0, 0))
    sums, cols, scales, info, bt, deltas = pl.pallas_call(
        first_kernel,
        grid=(4,),
        in_specs=[
            pl.BlockSpec(memory_space=pltpu.SMEM), whole((16, tok)), whole((1, 16)),
            whole((1, 16)), whole((1, 16)), quarter,
            narrow, narrow, whole((segs, 32, 128)),
        ],
        out_specs=[
            whole((segs, 72, 128)), narrow, narrow, whole((4, 16, tok)), turn, states,
        ],
        out_shape=(
            shape(segs, 72, 128), shape(tok, 128), shape(tok, 128, dtype=bf16),
            shape(4, 16, tok), shape(blocks, 128, Q, dtype=bf16), shape(4, blocks, 128, 256),
        ),
        scratch_shapes=[pltpu.VMEM((128, 128), f32), pltpu.VMEM((blocks, 128, Q), bf16)],
        compiler_params=arbitrary,
        cost_estimate=cost(10**9, 10**7),
        name="first",
    )(
        segment_slot, step_raw.T, log_rate[None], step_bias[None], skip_gain[None], out_grad, b_proj, c_proj,
        saved_states.reshape(segs, 32, 128),
    )
    sums = lax.all_to_all(sums, "seq", split_axis=0, concat_axis=0, tiled=True)

    def pairs(begin, steps, *before):
        last = len(before) > 0
        shifted = pl.BlockSpec((tok, 256), lambda g: (0, g + begin))
        info_part = pl.BlockSpec((1, 16, tok), lambda g: (g + begin, 0, 0))
        square = whole((blocks, Q, Q))
        hbm = pl.BlockSpec(memory_space=pl.ANY)

        def kernel(*refs):
            ins, outs = list(refs[:6]), list(refs[6:])
            if last:
                ins, outs = ins + [outs[0]], outs[3:]
            else:
                ins, outs = ins + [None], outs[:3] + [None, None] + outs[3:]
            pair_kernel(begin, *ins, *outs)

        return pl.pallas_call(
            kernel,
            grid=(steps,),
            in_specs=[shifted, shifted, narrow, narrow, narrow, info_part]
            + [square, hbm, hbm] * last,
            out_specs=[
                pl.BlockSpec((1, tok, 256), lambda g: (g + begin, 0, 0)),
                square,
                pl.BlockSpec((1, 8, tok), lambda g: (g + begin, 0, 0)),
            ]
            + [narrow, narrow] * last,
            out_shape=[shape(4, tok, 256), shape(blocks, Q, Q), shape(4, 8, tok)]
            + [shape(tok, 128)] * (2 * last),
            scratch_shapes=[pltpu.VMEM((blocks, Q, Q), f32)],
            input_output_aliases={7: 0, 8: 2} if last else {},
            compiler_params=arbitrary,
            cost_estimate=cost(5 * 10**9 * steps, 10**6 * steps),
            name="pairs",
        )(inputs, out_grad, b_proj, c_proj, cols, info, *before)

    adj, tot, pair_rows = pairs(0, LEFT)
    sums, tot = lax.optimization_barrier((sums, tot))
    carried, *starts = pl.pallas_call(
        carry_kernel,
        grid=(1,),
        in_specs=[whole((segs, 72, 128))],
        out_specs=[whole((segs, 32, 128))] + [whole((8, 32, 128))] * 4,
        out_shape=[shape(segs, 32, 128)] + [shape(8, 32, 128)] * 4,
        compiler_params=pltpu.CompilerParams(vmem_limit_bytes=8 * 2**20),
        cost_estimate=cost(10**6, 10**6),
        name="carry",
    )(sums)
    starts = [around(start, d) for d, start in enumerate(starts)]
    carried, tot = lax.optimization_barrier((carried, tot))
    incoming = lax.all_to_all(carried, "seq", split_axis=0, concat_axis=0, tiled=True)
    adj, tot, pair_rows, gb, gc = pairs(LEFT, 4 - LEFT, tot, adj, pair_rows)
    gc, rows, end = pl.pallas_call(
        forward_kernel,
        grid=(4,),
        in_specs=[
            quarter, quarter, narrow, turn, narrow,
            *[pl.BlockSpec((2, 32, 128), lambda g: (g, 0, 0))] * 4, narrow,
        ],
        out_specs=[narrow, rows8, state],
        out_shape=(
            shape(tok, 128), shape(4, 8, tok), shape(4, 128, 256),
        ),
        scratch_shapes=[
            pltpu.VMEM((256, 128), f32), pltpu.VMEM((tok, 256), f32), pltpu.VMEM((tok, 256), f32)
        ],
        compiler_params=arbitrary,
        cost_estimate=cost(3 * 10**9, 10**7),
        name="forward",
    )(inputs, out_grad, c_proj, bt, scales, *starts, gc)
    gc = lax.all_to_all(
        gc.reshape(4, tok // 4, 128), "head", split_axis=0, concat_axis=0, tiled=True
    ).sum(axis=0)
    grad_inputs, grad_step_raw, *gbs = pl.pallas_call(
        backward_kernel,
        grid=(4,),
        in_specs=[
            quarter, quarter, narrow, narrow, narrow, whole((4, 16, tok)), states,
            block, narrow, rows8,
            rows8, state,
            pl.BlockSpec((16, 1, 16, 128), lambda g: (0, g // 2, g % 2, 0)),
        ],
        out_specs=[quarter, whole((16, tok))] + [whole((tok // 4, 128))] * 4,
        out_shape=[shape(tok, 1024, dtype=bf16), shape(16, tok)] + [shape(tok // 4, 128)] * 4,
        scratch_shapes=[
            pltpu.VMEM((tok, 128), f32), pltpu.VMEM((4, 8, tok), f32), pltpu.VMEM((4, 4, Q), f32), pltpu.VMEM((tok, 256), f32)
        ],
        compiler_params=arbitrary,
        cost_estimate=cost(3 * 10**9, 10**7),
        name="backward",
    )(
        inputs, out_grad, b_proj, cols, scales, info, deltas, adj, gb, pair_rows, rows,
        end, incoming.reshape(16, 2, 32, 128),
    )
    far = around(gbs[2], 2)
    gb = gbs[0] + around(gbs[1], 1) + around(gbs[3], 3) + far
    return grad_inputs, grad_step_raw.T, gb, gc


def solution(mesh):
    return jax.shard_map(
        on_device,
        mesh=mesh,
        in_specs=(
            P("seq", "head"),
            P("seq", "head"),
            P("seq", None),
            P("seq", None),
            P("seq", "head"),
            P("head"),
            P("head"),
            P("head"),
            P(None, "seq", "head", None),
            P(),
        ),
        out_specs=(P("seq", "head"), P("seq", "head"), P(("seq", "head"), None), P(("seq", "head"), None)),
        check_vma=False,
    )
```

```python
import jax
import jax.numpy as jnp
from jax import lax
from jax.experimental import pallas as pl
from jax.experimental.pallas import tpu as pltpu
from jax.sharding import PartitionSpec as P

f32 = jnp.float32
bf16 = jnp.bfloat16
Q = 128
LOG2E = 1.4426950408889634
HIGHEST = lax.Precision.HIGHEST


def dn(a, b, precision=None):
    return lax.dot_general(
        a, b, (((1,), (0,)), ((), ())), precision=precision, preferred_element_type=f32
    )


def dt(a, b, precision=None):
    return lax.dot_general(
        a, b, (((1,), (1,)), ((), ())), precision=precision, preferred_element_type=f32
    )


def split(value):
    high = value.astype(bf16)
    low = (value - high.astype(f32)).astype(bf16)
    return high, low


def side(*parts):
    return jnp.concatenate(parts, axis=1)


def stack(*parts):
    return jnp.concatenate(parts, axis=0)


def spread(cols, base):
    rows = cols.shape[0]
    first = lax.broadcasted_iota(jnp.int32, (rows, 128), 1) < 64
    parts = []
    for j in range(2):
        left, right = (
            jnp.broadcast_to(cols[:, k : k + 1], (rows, 128))
            for k in (base + 2 * j, base + 2 * j + 1)
        )
        parts.append(jnp.where(first, left, right))
    return side(*parts)


def group_cols(cols, group):
    return pltpu.roll(cols, (128 - 4 * group) % 128, 1)


def head_sums(product):
    rows = []
    for j in range(2):
        turned = product[:, 128 * j : 128 * j + 128].T
        for i in range(2):
            part = turned[64 * i : 64 * i + 64]
            eight = part[0:8]
            for r in range(1, 8):
                eight = eight + part[8 * r : 8 * r + 8]
            rows.append(jnp.sum(eight, axis=0, keepdims=True))
    return stack(*rows)


GROW, SHRINK = 0, 32
LOGCOL, GROW_ALL, SKIP = (16 * q for q in range(3))


def repeater(base, group):
    row = lax.broadcasted_iota(jnp.int32, (128, 256), 0) - (base + 4 * group)
    head = lax.broadcasted_iota(jnp.int32, (128, 256), 1) // 64
    return jnp.where((row == head) | (row == head + 16), 1.0, 0.0).astype(bf16)


def first_kernel(
    slot_ref, raw_ref, rate_ref, bias_ref, skip_ref, dy_ref, b_ref, c_ref, saved_ref,
    sums_ref, cols_ref, scales_ref, info_ref, bt_ref, ct_ref,
    pad_ref,
):
    g = pl.program_id(0)
    blocks = dy_ref.shape[0] // Q

    @pl.when(g == 0)
    def prepare():
        for k in range(saved_ref.shape[0]):
            sums_ref[slot_ref[k], 40:72, :] = saved_ref[k]
        pad_ref[0:8, 0:16] = jnp.broadcast_to(jnp.exp(rate_ref[...]), (8, 16))
        pad_ref[8:16, 0:16] = jnp.broadcast_to(bias_ref[...], (8, 16))
        pad_ref[16:24, 0:16] = jnp.broadcast_to(skip_ref[...], (8, 16))
        small = pad_ref[...].T
        rate, bias, skip = (
            jnp.broadcast_to(small[0:16, k : k + 1], (16, Q)) for k in (0, 8, 16)
        )
        row = lax.broadcasted_iota(jnp.int32, (Q, Q), 0)
        lane = lax.broadcasted_iota(jnp.int32, (Q, Q), 1)
        upper = jnp.where(row <= lane, 1.0, 0.0)
        steps, gates, decays = [], [], []
        for k in range(blocks):
            z = raw_ref[:, k * Q : (k + 1) * Q] + bias
            small_exp = jnp.exp(-jnp.abs(z))
            step = jnp.maximum(z, 0.0) + jnp.log1p(small_exp)
            gates.append(jnp.where(z >= 0.0, 1.0, small_exp) / (1.0 + small_exp))
            steps.append(step)
            decays.append(-rate * step * LOG2E)
        sums = dn(stack(*decays), upper, HIGHEST)
        logs = [sums[16 * k : 16 * k + 16] for k in range(blocks)]
        ends = [log[:, Q - 1 : Q] for log in logs]
        so_far = jnp.zeros_like(ends[0])
        fill = jnp.zeros((80, Q), f32)
        fill_scales = jnp.zeros((64, Q), f32)
        for k in range(blocks):
            log, step = logs[k], steps[k]
            cols_ref[k * Q : (k + 1) * Q, :] = stack(
                log - jnp.log(step) * LOG2E,
                jnp.exp2(log + so_far),
                skip,
                fill,
            ).T
            grow, shrink = jnp.exp2(log), step * jnp.exp2(ends[k] - log)
            grow_high, shrink_high = (
                part.astype(bf16).astype(f32) for part in (grow, shrink)
            )
            scales_ref[k * Q : (k + 1) * Q, :] = stack(
                grow_high, grow - grow_high, shrink_high, shrink - shrink_high, fill_scales
            ).T.astype(bf16)
            so_far = so_far + ends[k]
            for r in range(4):
                four = slice(4 * r, 4 * r + 4)
                info_ref[r, :, k * Q : (k + 1) * Q] = stack(
                    log[four], step[four], gates[k][four], rate[four]
                )
            ct_ref[k] = c_ref[k * Q : (k + 1) * Q, :].astype(f32).T.astype(bf16)
            bt_ref[k] = b_ref[k * Q : (k + 1) * Q, :].astype(f32).T.astype(bf16)
        zero_rows = jnp.zeros((4, 128), f32)
        ends_row = []
        for r in range(4):
            last = spread(cols_ref[blocks * Q - 8 : blocks * Q, :], GROW_ALL + 4 * r)[7:8, :]
            ends_row += [last[:, 0:128], last[:, 128:256]]
        for half in range(2):
            tile = stack(*ends_row[4 * half : 4 * half + 4], zero_rows)
            for i in range(16):
                sums_ref[2 * i + half, 32:40, :] = tile

    total = jnp.zeros((128, 256), f32)
    before = None
    grow_to = repeater(GROW, g)
    for k in range(blocks):
        rows = slice(k * Q, (k + 1) * Q)
        grow = dn(scales_ref[rows, :], grow_to)
        high, low = split(dy_ref[rows, :].astype(f32) * grow)
        ct = ct_ref[k]
        delta = dn(side(ct, ct), stack(high, low))
        end = grow[Q - 1 : Q, :]
        total = delta if k == 0 else total + before * delta
        before = end if k == 0 else before * end
    at = pl.ds(pl.multiple_of((g % 2) * 16, 16), 16)
    for i in range(16):
        part = total[8 * i : 8 * i + 8]
        sums_ref[2 * i + g // 2, at, :] = stack(part[:, 0:128], part[:, 128:256])


def carry_kernel(sums_ref, out_ref, *start_refs):
    here = lax.axis_index("head")
    for d in range(4):
        group = lax.rem(here + d, 4)
        start_refs[d][...] = sums_ref[pl.ds(pl.multiple_of(group * 8, 8), 8), 40:72, :]
    carried = [jnp.zeros((8, 128), f32) for _ in range(4)]
    for m in reversed(range(sums_ref.shape[0])):
        for r in range(4):
            tile = slice(8 * r, 8 * r + 8)
            out_ref[m, tile, :] = carried[r]
            decay = jnp.broadcast_to(sums_ref[m, 32 + r : 33 + r, :], (8, 128))
            carried[r] = sums_ref[m, tile, :] + decay * carried[r]


def pair_kernel(
    x_ref, dy_ref, b_ref, c_ref, bt_ref, ct_ref, cols_ref, scales_ref, info_ref,
    adj_ref, rows_ref, into_ref, back_ref, gb_ref, gc_ref,
    tot_ref, meet_ref, scale_ref,
):
    g = pl.program_id(0)
    blocks = x_ref.shape[0] // Q

    @pl.when(g == 0)
    def clear():
        for k in range(blocks):
            rows = slice(k * Q, (k + 1) * Q)
            meet_ref[k] = dt(b_ref[rows, :], c_ref[rows, :])
        tot_ref[...] = jnp.zeros_like(tot_ref)

    skip = spread(group_cols(cols_ref[0:8, :], g), SKIP)[0:1, :]
    for source_ref, base, turn_ref, out_ref in (
        (x_ref, SHRINK, bt_ref, into_ref),
        (dy_ref, GROW, ct_ref, back_ref),
    ):
        scale_ref[...] = dn(scales_ref[...], repeater(base, g))
        for k in range(blocks):
            rows = slice(k * Q, (k + 1) * Q)
            high, low = split(source_ref[rows, :].astype(f32) * scale_ref[rows, :])
            turn = turn_ref[k]
            out_ref[0, k] = dn(side(turn, turn), stack(high, low))

    upper = lax.broadcasted_iota(jnp.int32, (Q, Q), 0) <= lax.broadcasted_iota(
        jnp.int32, (Q, Q), 1
    )
    lane = lax.broadcasted_iota(jnp.int32, (1, 128), 1)
    masks = [
        jnp.where(lane < 64, 1.0, 0.0).astype(bf16),
        jnp.where(lane < 64, 0.0, 1.0).astype(bf16),
    ]

    def one(k):
        rows = pl.ds(pl.multiple_of(k * Q, Q), Q)
        cols = group_cols(cols_ref[rows, :], g)
        meet = meet_ref[k]
        total = tot_ref[k]
        in_rows, products = [], []
        for j in range(2):
            lanes = slice(128 * j, 128 * j + 128)
            x_pair, dy_pair = x_ref[rows, lanes], dy_ref[rows, lanes]
            dots = dt(stack(x_pair * masks[0], x_pair * masks[1]), dy_pair)
            weights, values = [], []
            for i in range(2):
                h = 2 * j + i
                gap = info_ref[0, h : h + 1, rows] - jnp.broadcast_to(
                    cols[:, LOGCOL + h : LOGCOL + h + 1], (Q, Q)
                )
                decay = jnp.exp2(jnp.where(upper, gap, -1e30))
                pair = dots[Q * i : Q * i + Q] * decay
                total = total + pair
                in_rows.append(jnp.sum(pair * meet, axis=0, keepdims=True))
                weights += list(split(decay * meet))
                values += [dy_pair * masks[i]] * 2
            adj = dn(side(*weights), stack(*values))
            adj_ref[0, rows, lanes] = adj + skip[:, lanes] * dy_pair.astype(f32)
            products.append(x_pair.astype(f32) * adj)
        tot_ref[k] = total
        rows_ref[0, 0:4, rows] = stack(*in_rows)
        rows_ref[0, 4:8, rows] = head_sums(side(*products))

    def some(i, unused):
        for k in range(PAIR_UNROLL):
            one(i * PAIR_UNROLL + k)
        return unused

    lax.fori_loop(0, blocks // PAIR_UNROLL, some, 0)

    @pl.when(g == pl.num_programs(0) - 1)
    def finish():
        for k in range(blocks):
            rows = slice(k * Q, (k + 1) * Q)
            total = tot_ref[k]
            high, low = split(total)
            c = c_ref[rows, :]
            gb_ref[rows, :] = dn(side(high, low), stack(c, c))
            high, low = split(total.T)
            b = b_ref[rows, :]
            gc_ref[rows, :] = dn(side(high, low), stack(b, b))


PAIR_UNROLL = 8


def three(rows_high, rows_low, high, low):
    both = dt(rows_high, stack(high, low))
    return both[:, 0:128] + both[:, 128:256] + dt(rows_low, high)


def forward_kernel(
    dy_ref, c_ref, into_ref, scales_ref, start0_ref, start1_ref, start2_ref, start3_ref, gc_in_ref,
    gc_ref, rows_ref, end_ref,
    hold_ref, grow_ref,
):
    g = pl.program_id(0)
    blocks = dy_ref.shape[0] // Q

    @pl.when(g == 0)
    def copy():
        gc_ref[...] = gc_in_ref[...]

    here = lax.axis_index("head")
    for d, start_ref in enumerate((start0_ref, start1_ref, start2_ref, start3_ref)):
        part = lax.rem(here + 4 - d, 4)
        for h in range(4):
            at = 16 * (h % 2)
            to = pl.ds(pl.multiple_of(64 * h + 16 * part, 16), 16)
            hold_ref[to, :] = start_ref[h // 2, at : at + 16, :]
    state = hold_ref[...].T
    grow_ref[...] = dn(scales_ref[...], repeater(GROW, g))
    for k in range(blocks):
        rows = slice(k * Q, (k + 1) * Q)
        grow = grow_ref[rows, :]
        s_high, s_low = split(state)
        c = c_ref[rows, :]
        from_state = dn(side(c, c), stack(s_high, s_low))
        dy_grown = dy_ref[rows, :].astype(f32) * grow
        dy_high, dy_low = split(dy_grown)
        rows_ref[0, 0:4, rows] = head_sums(dy_grown * from_state)
        gc_ref[rows, :] += three(dy_high, dy_low, s_high, s_low)
        state = grow[Q - 1 : Q, :] * state + into_ref[0, k]
    end_ref[0] = state


def backward_kernel(
    x_ref, b_ref, scales_ref, info_ref, back_ref, adj_ref, gb_in_ref,
    pair_rows_ref, rows_ref, end_ref, in_ref,
    gx_ref, raw_ref, gb0_ref, gb1_ref, gb2_ref, gb3_ref,
    gb_ref, keep_ref, through_ref, shrink_ref,
):
    g = pl.program_id(0)
    blocks = x_ref.shape[0] // Q

    @pl.when(g == 0)
    def copy():
        gb_ref[...] = gb_in_ref[...]

    adjoint = side(*[in_ref[:, 0, 8 * r : 8 * r + 8, :].reshape(128, 128) for r in range(2)])
    meeting = jnp.sum(adjoint * end_ref[0], axis=0, keepdims=True)
    row = lax.broadcasted_iota(jnp.int32, (8, 256), 0)
    lane = lax.broadcasted_iota(jnp.int32, (8, 256), 1)
    through = jnp.sum(jnp.where(row == lane // 64, meeting, 0.0), axis=1, keepdims=True)[0:4]
    shrink_ref[...] = dn(scales_ref[...], repeater(SHRINK, g))
    ends = stack(*[scales_ref[k * Q + Q - 16 : k * Q + Q, :] for k in range(blocks)])
    decays = dn(ends, repeater(GROW, g))
    for k in reversed(range(blocks)):
        rows = slice(k * Q, (k + 1) * Q)
        shrink = shrink_ref[rows, :]
        x_full = x_ref[rows, :].astype(f32)
        x_high, x_low = split(x_full * shrink)
        g_high, g_low = split(adjoint)
        b = b_ref[rows, :]
        adj = shrink * dn(side(b, b), stack(g_high, g_low))
        gx_ref[rows, :] = (adj_ref[0, rows, :] + adj).astype(bf16)
        out_rows = pair_rows_ref[0, 4:8, rows] + head_sums(x_full * adj)
        gb_ref[rows, :] += three(x_high, x_low, g_high, g_low)
        adjoint = decays[16 * k + 15 : 16 * k + 16, :] * adjoint + back_ref[0, k]
        keep_ref[g, 0:4, rows] = (
            pair_rows_ref[0, 0:4, rows] + rows_ref[0, 0:4, rows] - out_rows
        )
        keep_ref[g, 4:8, rows] = out_rows
    through_ref[g] = jnp.broadcast_to(through, (4, Q))

    @pl.when(g == pl.num_programs(0) - 1)
    def finish():
        here = lax.axis_index("head")
        for d, part_ref in enumerate((gb0_ref, gb1_ref, gb2_ref, gb3_ref)):
            size = part_ref.shape[0]
            at = lax.rem(here + d, 4) * size
            part_ref[...] = gb_ref[pl.ds(pl.multiple_of(at, size), size), :]
        after = jnp.where(
            lax.broadcasted_iota(jnp.int32, (Q, Q), 0)
            >= lax.broadcasted_iota(jnp.int32, (Q, Q), 1),
            1.0, 0.0,
        )

        def all_heads(ref, first, rows):
            return stack(*[ref[r, first : first + 4, rows] for r in range(4)])

        parts = [all_heads(keep_ref, 0, slice(k * Q, (k + 1) * Q)) for k in range(blocks)]
        sums = dn(stack(*parts), after, HIGHEST)
        later = stack(*[through_ref[r][:, 0:1] for r in range(4)])
        for k in reversed(range(blocks)):
            rows = slice(k * Q, (k + 1) * Q)
            here = sums[16 * k : 16 * k + 16]
            step, gate, rate = (all_heads(info_ref, 4 * r, rows) for r in (1, 2, 3))
            x_adj = all_heads(keep_ref, 4, rows)
            raw_ref[:, rows] = gate * (x_adj / step - rate * (here + later))
            later = later + here[:, 0:1]


def whole(shape):
    zeros = (0,) * len(shape)
    return pl.BlockSpec(tuple(shape), lambda g, zeros=zeros: zeros)


def around(array, distance):
    if distance == 0:
        return array
    heads = lax.axis_size("head")
    return lax.ppermute(array, "head", [(i, (i + distance) % heads) for i in range(heads)])


def on_device(
    inputs, out_grad, b_proj, c_proj, step_raw, log_rate, step_bias, skip_gain,
    saved_states, segment_slot,
):
    tok = inputs.shape[0]
    blocks = tok // Q
    segs = saved_states.shape[0]
    arbitrary = pltpu.CompilerParams(dimension_semantics=("arbitrary",))

    def shape(*dims, dtype=f32):
        return jax.ShapeDtypeStruct(dims, dtype)

    def cost(flops, bytes_accessed):
        return pl.CostEstimate(
            flops=flops, transcendentals=0, bytes_accessed=bytes_accessed
        )

    quarter = pl.BlockSpec((tok, 256), lambda g: (0, g))
    narrow = whole((tok, 128))
    rows8 = pl.BlockSpec((1, 8, tok), lambda g: (g, 0, 0))
    info_spec = pl.BlockSpec((1, 16, tok), lambda g: (g, 0, 0))
    turn = whole((blocks, 128, Q))
    states = pl.BlockSpec((1, blocks, 128, 256), lambda g: (g, 0, 0, 0))
    block = pl.BlockSpec((1, tok, 256), lambda g: (g, 0, 0))
    state = pl.BlockSpec((1, 128, 256), lambda g: (g, 0, 0))
    sums, cols, scales, info, bt, ct = pl.pallas_call(
        first_kernel,
        grid=(4,),
        in_specs=[
            pl.BlockSpec(memory_space=pltpu.SMEM), whole((16, tok)), whole((1, 16)),
            whole((1, 16)), whole((1, 16)), quarter,
            narrow, narrow, whole((segs, 32, 128)),
        ],
        out_specs=[
            whole((segs, 72, 128)), narrow, narrow, whole((4, 16, tok)), turn, turn,
        ],
        out_shape=(
            shape(segs, 72, 128), shape(tok, 128), shape(tok, 128, dtype=bf16),
            shape(4, 16, tok), shape(blocks, 128, Q, dtype=bf16),
            shape(blocks, 128, Q, dtype=bf16),
        ),
        scratch_shapes=[pltpu.VMEM((128, 128), f32)],
        compiler_params=arbitrary,
        cost_estimate=cost(10**9, 10**7),
        name="first",
    )(
        segment_slot, step_raw.T, log_rate[None], step_bias[None], skip_gain[None], out_grad, b_proj, c_proj,
        saved_states.reshape(segs, 32, 128),
    )
    sums = lax.all_to_all(sums, "seq", split_axis=0, concat_axis=0, tiled=True)

    adj, pair_rows, into, back, gb, gc = pl.pallas_call(
        pair_kernel,
        grid=(4,),
        in_specs=[
            quarter, quarter, narrow, narrow, turn, turn, narrow, narrow, info_spec
        ],
        out_specs=[block, rows8, states, states, narrow, narrow],
        out_shape=[
            shape(4, tok, 256), shape(4, 8, tok), shape(4, blocks, 128, 256),
            shape(4, blocks, 128, 256), shape(tok, 128), shape(tok, 128),
        ],
        scratch_shapes=[
            pltpu.VMEM((blocks, Q, Q), f32), pltpu.VMEM((blocks, Q, Q), f32),
            pltpu.VMEM((tok, 256), f32),
        ],
        compiler_params=arbitrary,
        cost_estimate=cost(2 * 10**10, 10**7),
        name="pairs",
    )(inputs, out_grad, b_proj, c_proj, bt, ct, cols, scales, info)
    sums, gb = lax.optimization_barrier((sums, gb))
    carried, *starts = pl.pallas_call(
        carry_kernel,
        grid=(1,),
        in_specs=[whole((segs, 72, 128))],
        out_specs=[whole((segs, 32, 128))] + [whole((8, 32, 128))] * 4,
        out_shape=[shape(segs, 32, 128)] + [shape(8, 32, 128)] * 4,
        compiler_params=pltpu.CompilerParams(vmem_limit_bytes=8 * 2**20),
        cost_estimate=cost(10**6, 10**6),
        name="carry",
    )(sums)
    shifted = []
    for d, start in enumerate(starts):
        shifted.append(around(start, d))
    incoming = lax.all_to_all(carried, "seq", split_axis=0, concat_axis=0, tiled=True)
    gc, rows, end = pl.pallas_call(
        forward_kernel,
        grid=(4,),
        in_specs=[
            quarter, narrow, states, narrow,
            *[pl.BlockSpec((2, 32, 128), lambda g: (g, 0, 0))] * 4, narrow,
        ],
        out_specs=[narrow, rows8, state],
        out_shape=(
            shape(tok, 128), shape(4, 8, tok), shape(4, 128, 256),
        ),
        scratch_shapes=[
            pltpu.VMEM((256, 128), f32), pltpu.VMEM((tok, 256), f32)
        ],
        compiler_params=arbitrary,
        cost_estimate=cost(3 * 10**9, 10**7),
        name="forward",
    )(out_grad, c_proj, into, scales, *shifted, gc)
    gc = lax.all_to_all(
        gc.reshape(4, tok // 4, 128), "head", split_axis=0, concat_axis=0, tiled=True
    ).sum(axis=0)
    grad_inputs, grad_step_raw, *gbs = pl.pallas_call(
        backward_kernel,
        grid=(4,),
        in_specs=[
            quarter, narrow, narrow, whole((4, 16, tok)), states,
            block, narrow, rows8,
            rows8, state,
            pl.BlockSpec((16, 1, 16, 128), lambda g: (0, g // 2, g % 2, 0)),
        ],
        out_specs=[quarter, whole((16, tok))] + [whole((tok // 4, 128))] * 4,
        out_shape=[shape(tok, 1024, dtype=bf16), shape(16, tok)] + [shape(tok // 4, 128)] * 4,
        scratch_shapes=[
            pltpu.VMEM((tok, 128), f32), pltpu.VMEM((4, 8, tok), f32), pltpu.VMEM((4, 4, Q), f32), pltpu.VMEM((tok, 256), f32)
        ],
        compiler_params=arbitrary,
        cost_estimate=cost(3 * 10**9, 10**7),
        name="backward",
    )(
        inputs, b_proj, scales, info, back, adj, gb, pair_rows, rows,
        end, incoming.reshape(16, 2, 32, 128),
    )
    far = around(gbs[2], 2)
    gb = gbs[0] + around(gbs[1], 1) + around(gbs[3], 3) + far
    return grad_inputs, grad_step_raw.T, gb, gc


def solution(mesh):
    return jax.shard_map(
        on_device,
        mesh=mesh,
        in_specs=(
            P("seq", "head"),
            P("seq", "head"),
            P("seq", None),
            P("seq", None),
            P("seq", "head"),
            P("head"),
            P("head"),
            P("head"),
            P(None, "seq", "head", None),
            P(),
        ),
        out_specs=(P("seq", "head"), P("seq", "head"), P(("seq", "head"), None), P(("seq", "head"), None)),
        check_vma=False,
    )
```

```python
import jax
import jax.numpy as jnp
from jax import lax
from jax.experimental import pallas as pl
from jax.experimental.pallas import tpu as pltpu
from jax.sharding import PartitionSpec as P

f32 = jnp.float32
bf16 = jnp.bfloat16
Q = 128
LOG2E = 1.4426950408889634
HIGHEST = lax.Precision.HIGHEST


def dn(a, b, precision=None):
    return lax.dot_general(
        a, b, (((1,), (0,)), ((), ())), precision=precision, preferred_element_type=f32
    )


def dt(a, b, precision=None):
    return lax.dot_general(
        a, b, (((1,), (1,)), ((), ())), precision=precision, preferred_element_type=f32
    )


def split(value):
    high = value.astype(bf16)
    low = (value - high.astype(f32)).astype(bf16)
    return high, low


def side(*parts):
    return jnp.concatenate(parts, axis=1)


def stack(*parts):
    return jnp.concatenate(parts, axis=0)


def spread(cols, base):
    rows = cols.shape[0]
    first = lax.broadcasted_iota(jnp.int32, (rows, 128), 1) < 64
    parts = []
    for j in range(2):
        left, right = (
            jnp.broadcast_to(cols[:, k : k + 1], (rows, 128))
            for k in (base + 2 * j, base + 2 * j + 1)
        )
        parts.append(jnp.where(first, left, right))
    return side(*parts)


def group_cols(cols, group):
    return pltpu.roll(cols, (128 - 4 * group) % 128, 1)


def head_sums(product):
    rows = []
    for j in range(2):
        turned = product[:, 128 * j : 128 * j + 128].T
        for i in range(2):
            part = turned[64 * i : 64 * i + 64]
            eight = part[0:8]
            for r in range(1, 8):
                eight = eight + part[8 * r : 8 * r + 8]
            rows.append(jnp.sum(eight, axis=0, keepdims=True))
    return stack(*rows)


GROW, SHRINK, GROW_ALL = 0, 32, 64
LOGCOL, SKIP = 0, 16


def repeater(base, group):
    row = lax.broadcasted_iota(jnp.int32, (128, 256), 0) - (base + 4 * group)
    head = lax.broadcasted_iota(jnp.int32, (128, 256), 1) // 64
    return jnp.where((row == head) | (row == head + 16), 1.0, 0.0).astype(bf16)


def first_kernel(
    slot_ref, raw_ref, rate_ref, bias_ref, skip_ref, dy_ref, c_ref, saved_ref,
    sums_ref, scales_ref, info_ref,
    pad_ref, ct_ref,
):
    g = pl.program_id(0)
    blocks = dy_ref.shape[0] // Q

    @pl.when(g == 0)
    def prepare():
        for k in range(saved_ref.shape[0]):
            sums_ref[slot_ref[k], 40:72, :] = saved_ref[k]
        pad_ref[0:8, 0:16] = jnp.broadcast_to(jnp.exp(rate_ref[...]), (8, 16))
        pad_ref[8:16, 0:16] = jnp.broadcast_to(bias_ref[...], (8, 16))
        pad_ref[16:24, 0:16] = jnp.broadcast_to(skip_ref[...], (8, 16))
        small = pad_ref[...].T
        rate, bias, skip = (
            jnp.broadcast_to(small[0:16, k : k + 1], (16, Q)) for k in (0, 8, 16)
        )
        row = lax.broadcasted_iota(jnp.int32, (Q, Q), 0)
        lane = lax.broadcasted_iota(jnp.int32, (Q, Q), 1)
        upper = jnp.where(row <= lane, 1.0, 0.0)
        steps, gates, decays = [], [], []
        for k in range(blocks):
            z = raw_ref[:, k * Q : (k + 1) * Q] + bias
            small_exp = jnp.exp(-jnp.abs(z))
            step = jnp.maximum(z, 0.0) + jnp.log1p(small_exp)
            gates.append(jnp.where(z >= 0.0, 1.0, small_exp) / (1.0 + small_exp))
            steps.append(step)
            decays.append(-rate * step * LOG2E)
        sums = dn(stack(*decays), upper, HIGHEST)
        logs = [sums[16 * k : 16 * k + 16] for k in range(blocks)]
        ends = [log[:, Q - 1 : Q] for log in logs]
        so_far = jnp.zeros_like(ends[0])
        fill = jnp.zeros((32, Q), f32)
        for k in range(blocks):
            log, step = logs[k], steps[k]
            parts = []
            for part in (
                jnp.exp2(log), step * jnp.exp2(ends[k] - log), jnp.exp2(log + so_far)
            ):
                high = part.astype(bf16).astype(f32)
                parts += [high, part - high]
            scales_ref[k * Q : (k + 1) * Q, :] = stack(*parts, fill).T.astype(bf16)
            so_far = so_far + ends[k]
            for r in range(4):
                four = slice(4 * r, 4 * r + 4)
                info_ref[r, :, k * Q : (k + 1) * Q] = stack(
                    log[four], step[four], gates[k][four], rate[four], skip[four], skip[four]
                )
            ct_ref[k] = c_ref[k * Q : (k + 1) * Q, :].astype(f32).T.astype(bf16)
        ends_row = []
        for r in range(4):
            last = dn(scales_ref[blocks * Q - 16 : blocks * Q, :], repeater(GROW_ALL, r))
            ends_row += [last[15:16, 0:128], last[15:16, 128:256]]
        for half in range(2):
            tile = stack(*ends_row[4 * half : 4 * half + 4], jnp.zeros((4, 128), f32))
            for i in range(16):
                sums_ref[2 * i + half, 32:40, :] = tile

    total = jnp.zeros((128, 256), f32)
    before = None
    grow_to = repeater(GROW, g)
    for k in range(blocks):
        rows = slice(k * Q, (k + 1) * Q)
        grow = dn(scales_ref[rows, :], grow_to)
        high, low = split(dy_ref[rows, :].astype(f32) * grow)
        ct = ct_ref[k]
        delta = dn(side(ct, ct), stack(high, low))
        end = grow[Q - 1 : Q, :]
        total = delta if k == 0 else total + before * delta
        before = end if k == 0 else before * end
    at = pl.ds(pl.multiple_of((g % 2) * 16, 16), 16)
    for i in range(16):
        part = total[8 * i : 8 * i + 8]
        sums_ref[2 * i + g // 2, at, :] = stack(part[:, 0:128], part[:, 128:256])


def carry_kernel(sums_ref, out_ref, *start_refs):
    here = lax.axis_index("head")
    for d in range(4):
        group = lax.rem(here + d, 4)
        start_refs[d][...] = sums_ref[pl.ds(pl.multiple_of(group * 8, 8), 8), 40:72, :]
    carried = [jnp.zeros((8, 128), f32) for _ in range(4)]
    for m in reversed(range(sums_ref.shape[0])):
        for r in range(4):
            tile = slice(8 * r, 8 * r + 8)
            out_ref[m, tile, :] = carried[r]
            decay = jnp.broadcast_to(sums_ref[m, 32 + r : 33 + r, :], (8, 128))
            carried[r] = sums_ref[m, tile, :] + decay * carried[r]


def pair_kernel(
    x_ref, dy_ref, b_ref, c_ref, scales_ref, info_ref,
    adj_ref, rows_ref, into_ref, back_ref, gb_ref, gc_ref,
    tot_ref, meet_ref, scale_ref, cols_ref, bt_ref, ct_ref,
):
    g = pl.program_id(0)
    blocks = x_ref.shape[0] // Q

    @pl.when(g == 0)
    def clear():
        for k in range(blocks):
            rows = slice(k * Q, (k + 1) * Q)
            meet_ref[k] = dt(b_ref[rows, :], c_ref[rows, :])
            ct_ref[k] = c_ref[rows, :].astype(f32).T.astype(bf16)
            bt_ref[k] = b_ref[rows, :].astype(f32).T.astype(bf16)
            logs = [
                info_ref[r, 0:4, rows] - jnp.log(info_ref[r, 4:8, rows]) * LOG2E for r in range(4)
            ]
            skips = [info_ref[r, 16:20, rows] for r in range(4)]
            cols_ref[rows, :] = stack(*logs, *skips, jnp.zeros((96, Q), f32)).T
        tot_ref[...] = jnp.zeros_like(tot_ref)

    skip = spread(group_cols(cols_ref[0:8, :], g), SKIP)[0:1, :]
    for source_ref, base, turn_ref, out_ref in (
        (x_ref, SHRINK, bt_ref, into_ref),
        (dy_ref, GROW, ct_ref, back_ref),
    ):
        scale_ref[...] = dn(scales_ref[...], repeater(base, g))
        for k in range(blocks):
            rows = slice(k * Q, (k + 1) * Q)
            high, low = split(source_ref[rows, :].astype(f32) * scale_ref[rows, :])
            turn = turn_ref[k]
            out_ref[0, k] = dn(side(turn, turn), stack(high, low))

    upper = lax.broadcasted_iota(jnp.int32, (Q, Q), 0) <= lax.broadcasted_iota(
        jnp.int32, (Q, Q), 1
    )
    lane = lax.broadcasted_iota(jnp.int32, (1, 128), 1)
    masks = [
        jnp.where(lane < 64, 1.0, 0.0).astype(bf16),
        jnp.where(lane < 64, 0.0, 1.0).astype(bf16),
    ]

    def one(k):
        rows = pl.ds(pl.multiple_of(k * Q, Q), Q)
        cols = group_cols(cols_ref[rows, :], g)
        meet = meet_ref[k]
        total = tot_ref[k]
        in_rows, products = [], []
        for j in range(2):
            lanes = slice(128 * j, 128 * j + 128)
            x_pair, dy_pair = x_ref[rows, lanes], dy_ref[rows, lanes]
            dots = dt(stack(x_pair * masks[0], x_pair * masks[1]), dy_pair)
            weights, values = [], []
            for i in range(2):
                h = 2 * j + i
                gap = info_ref[g, h : h + 1, rows] - jnp.broadcast_to(
                    cols[:, LOGCOL + h : LOGCOL + h + 1], (Q, Q)
                )
                decay = jnp.exp2(jnp.where(upper, gap, -1e30))
                pair = dots[Q * i : Q * i + Q] * decay
                total = total + pair
                in_rows.append(jnp.sum(pair * meet, axis=0, keepdims=True))
                weights += list(split(decay * meet))
                values += [dy_pair * masks[i]] * 2
            adj = dn(side(*weights), stack(*values))
            adj_ref[0, rows, lanes] = adj + skip[:, lanes] * dy_pair.astype(f32)
            products.append(x_pair.astype(f32) * adj)
        tot_ref[k] = total
        rows_ref[0, 0:4, rows] = stack(*in_rows)
        rows_ref[0, 4:8, rows] = head_sums(side(*products))

    def some(i, unused):
        for k in range(PAIR_UNROLL):
            one(i * PAIR_UNROLL + k)
        return unused

    lax.fori_loop(0, blocks // PAIR_UNROLL, some, 0)

    @pl.when(g == pl.num_programs(0) - 1)
    def finish():
        for k in range(blocks):
            rows = slice(k * Q, (k + 1) * Q)
            total = tot_ref[k]
            high, low = split(total)
            c = c_ref[rows, :]
            gb_ref[rows, :] = dn(side(high, low), stack(c, c))
            high, low = split(total.T)
            b = b_ref[rows, :]
            gc_ref[rows, :] = dn(side(high, low), stack(b, b))


PAIR_UNROLL = 8


def three(rows_high, rows_low, high, low):
    both = dt(rows_high, stack(high, low))
    return both[:, 0:128] + both[:, 128:256] + dt(rows_low, high)


def forward_kernel(
    dy_ref, c_ref, into_ref, scales_ref, start0_ref, start1_ref, start2_ref, start3_ref, gc_in_ref,
    gc_ref, rows_ref, end_ref,
    hold_ref, grow_ref,
):
    g = pl.program_id(0)
    blocks = dy_ref.shape[0] // Q

    @pl.when(g == 0)
    def copy():
        gc_ref[...] = gc_in_ref[...]

    here = lax.axis_index("head")
    for d, start_ref in enumerate((start0_ref, start1_ref, start2_ref, start3_ref)):
        part = lax.rem(here + 4 - d, 4)
        for h in range(4):
            at = 16 * (h % 2)
            to = pl.ds(pl.multiple_of(64 * h + 16 * part, 16), 16)
            hold_ref[to, :] = start_ref[h // 2, at : at + 16, :]
    state = hold_ref[...].T
    grow_ref[...] = dn(scales_ref[...], repeater(GROW, g))
    for k in range(blocks):
        rows = slice(k * Q, (k + 1) * Q)
        grow = grow_ref[rows, :]
        s_high, s_low = split(state)
        c = c_ref[rows, :]
        from_state = dn(side(c, c), stack(s_high, s_low))
        dy_grown = dy_ref[rows, :].astype(f32) * grow
        dy_high, dy_low = split(dy_grown)
        rows_ref[0, 0:4, rows] = head_sums(dy_grown * from_state)
        gc_ref[rows, :] += three(dy_high, dy_low, s_high, s_low)
        state = grow[Q - 1 : Q, :] * state + into_ref[0, k]
    end_ref[0] = state


def backward_kernel(
    x_ref, scales_ref, back_ref, gb_in_ref, end_ref, in_ref,
    through_ref, gb0_ref, gb1_ref, gb2_ref, gb3_ref,
    gb_ref, shrink_ref,
):
    g = pl.program_id(0)
    blocks = x_ref.shape[0] // Q

    @pl.when(g == 0)
    def copy():
        gb_ref[...] = gb_in_ref[...]

    adjoint = side(*[in_ref[:, 0, 8 * r : 8 * r + 8, :].reshape(128, 128) for r in range(2)])
    meeting = jnp.sum(adjoint * end_ref[0], axis=0, keepdims=True)
    row = lax.broadcasted_iota(jnp.int32, (8, 256), 0)
    lane = lax.broadcasted_iota(jnp.int32, (8, 256), 1)
    through = jnp.sum(jnp.where(row == lane // 64, meeting, 0.0), axis=1, keepdims=True)
    through_ref[0] = jnp.broadcast_to(through, (8, 128))
    shrink_ref[...] = dn(scales_ref[...], repeater(SHRINK, g))
    ends = stack(*[scales_ref[k * Q + Q - 16 : k * Q + Q, :] for k in range(blocks)])
    decays = dn(ends, repeater(GROW, g))
    for k in reversed(range(blocks)):
        rows = slice(k * Q, (k + 1) * Q)
        x_high, x_low = split(x_ref[rows, :].astype(f32) * shrink_ref[rows, :])
        g_high, g_low = split(adjoint)
        gb_ref[rows, :] += three(x_high, x_low, g_high, g_low)
        adjoint = decays[16 * k + 15 : 16 * k + 16, :] * adjoint + back_ref[0, k]

    @pl.when(g == pl.num_programs(0) - 1)
    def finish():
        here = lax.axis_index("head")
        for d, part_ref in enumerate((gb0_ref, gb1_ref, gb2_ref, gb3_ref)):
            size = part_ref.shape[0]
            at = lax.rem(here + d, 4) * size
            part_ref[...] = gb_ref[pl.ds(pl.multiple_of(at, size), size), :]


def last_kernel(
    x_ref, b_ref, scales_ref, info_ref, adj_ref, pair_rows_ref, rows_ref,
    back_ref, in_ref, through_ref,
    gx_ref, raw_ref,
    keep_ref, shrink_ref,
):
    g = pl.program_id(0)
    blocks = x_ref.shape[0] // Q
    adjoint = side(*[in_ref[:, 0, 8 * r : 8 * r + 8, :].reshape(128, 128) for r in range(2)])
    shrink_ref[...] = dn(scales_ref[...], repeater(SHRINK, g))
    ends = stack(*[scales_ref[k * Q + Q - 16 : k * Q + Q, :] for k in range(blocks)])
    decays = dn(ends, repeater(GROW, g))
    for k in reversed(range(blocks)):
        rows = slice(k * Q, (k + 1) * Q)
        b = b_ref[rows, :]
        adj = shrink_ref[rows, :] * dn(side(b, b), stack(*split(adjoint)))
        adjoint = decays[16 * k + 15 : 16 * k + 16, :] * adjoint + back_ref[0, k]
        gx_ref[rows, :] = (adj_ref[0, rows, :] + adj).astype(bf16)
        out_rows = pair_rows_ref[0, 4:8, rows] + head_sums(x_ref[rows, :].astype(f32) * adj)
        keep_ref[g, 0:4, rows] = (
            pair_rows_ref[0, 0:4, rows] + rows_ref[0, 0:4, rows] - out_rows
        )
        keep_ref[g, 4:8, rows] = out_rows

    @pl.when(g == pl.num_programs(0) - 1)
    def finish():
        after = jnp.where(
            lax.broadcasted_iota(jnp.int32, (Q, Q), 0)
            >= lax.broadcasted_iota(jnp.int32, (Q, Q), 1),
            1.0, 0.0,
        )

        def all_heads(ref, first, rows):
            return stack(*[ref[r, first : first + 4, rows] for r in range(4)])

        parts = [all_heads(keep_ref, 0, slice(k * Q, (k + 1) * Q)) for k in range(blocks)]
        sums = dn(stack(*parts), after, HIGHEST)
        later = stack(*[through_ref[r, 0:4, 0:1] for r in range(4)])
        for k in reversed(range(blocks)):
            rows = slice(k * Q, (k + 1) * Q)
            here = sums[16 * k : 16 * k + 16]
            step, gate, rate = (all_heads(info_ref, 4 * r, rows) for r in (1, 2, 3))
            x_adj = all_heads(keep_ref, 4, rows)
            raw_ref[:, rows] = gate * (x_adj / step - rate * (here + later))
            later = later + here[:, 0:1]


def whole(shape):
    zeros = (0,) * len(shape)
    return pl.BlockSpec(tuple(shape), lambda g, zeros=zeros: zeros)


def around(array, distance):
    if distance == 0:
        return array
    heads = lax.axis_size("head")
    return lax.ppermute(array, "head", [(i, (i + distance) % heads) for i in range(heads)])


def on_device(
    inputs, out_grad, b_proj, c_proj, step_raw, log_rate, step_bias, skip_gain,
    saved_states, segment_slot,
):
    tok = inputs.shape[0]
    blocks = tok // Q
    segs = saved_states.shape[0]
    arbitrary = pltpu.CompilerParams(dimension_semantics=("arbitrary",))

    def shape(*dims, dtype=f32):
        return jax.ShapeDtypeStruct(dims, dtype)

    def cost(flops, bytes_accessed):
        return pl.CostEstimate(
            flops=flops, transcendentals=0, bytes_accessed=bytes_accessed
        )

    quarter = pl.BlockSpec((tok, 256), lambda g: (0, g))
    narrow = whole((tok, 128))
    rows8 = pl.BlockSpec((1, 8, tok), lambda g: (g, 0, 0))
    states = pl.BlockSpec((1, blocks, 128, 256), lambda g: (g, 0, 0, 0))
    block = pl.BlockSpec((1, tok, 256), lambda g: (g, 0, 0))
    state = pl.BlockSpec((1, 128, 256), lambda g: (g, 0, 0))
    sums, scales, info = pl.pallas_call(
        first_kernel,
        grid=(4,),
        in_specs=[
            pl.BlockSpec(memory_space=pltpu.SMEM), whole((16, tok)), whole((1, 16)),
            whole((1, 16)), whole((1, 16)), quarter, narrow, whole((segs, 32, 128)),
        ],
        out_specs=[whole((segs, 72, 128)), narrow, whole((4, 24, tok))],
        out_shape=(
            shape(segs, 72, 128), shape(tok, 128, dtype=bf16), shape(4, 24, tok),
        ),
        scratch_shapes=[pltpu.VMEM((128, 128), f32), pltpu.VMEM((blocks, 128, Q), bf16)],
        compiler_params=arbitrary,
        cost_estimate=cost(10**9, 10**7),
        name="first",
    )(
        segment_slot, step_raw.T, log_rate[None], step_bias[None], skip_gain[None], out_grad,
        c_proj, saved_states.reshape(segs, 32, 128),
    )
    sums = lax.all_to_all(sums, "seq", split_axis=0, concat_axis=0, tiled=True)

    adj, pair_rows, into, back, gb, gc = pl.pallas_call(
        pair_kernel,
        grid=(4,),
        in_specs=[
            quarter, quarter, narrow, narrow, narrow, whole((4, 24, tok))
        ],
        out_specs=[block, rows8, states, states, narrow, narrow],
        out_shape=[
            shape(4, tok, 256), shape(4, 8, tok), shape(4, blocks, 128, 256),
            shape(4, blocks, 128, 256), shape(tok, 128), shape(tok, 128),
        ],
        scratch_shapes=[
            pltpu.VMEM((blocks, Q, Q), f32), pltpu.VMEM((blocks, Q, Q), f32),
            pltpu.VMEM((tok, 256), f32), pltpu.VMEM((tok, 128), f32),
            pltpu.VMEM((blocks, 128, Q), bf16), pltpu.VMEM((blocks, 128, Q), bf16),
        ],
        compiler_params=arbitrary,
        cost_estimate=cost(2 * 10**10, 10**7),
        name="pairs",
    )(inputs, out_grad, b_proj, c_proj, scales, info)
    sums, gb = lax.optimization_barrier((sums, gb))
    carried, *starts = pl.pallas_call(
        carry_kernel,
        grid=(1,),
        in_specs=[whole((segs, 72, 128))],
        out_specs=[whole((segs, 32, 128))] + [whole((8, 32, 128))] * 4,
        out_shape=[shape(segs, 32, 128)] + [shape(8, 32, 128)] * 4,
        compiler_params=pltpu.CompilerParams(vmem_limit_bytes=8 * 2**20),
        cost_estimate=cost(10**6, 10**6),
        name="carry",
    )(sums)
    shifted = []
    for d, start in enumerate(starts):
        shifted.append(around(start, d))
    incoming = lax.all_to_all(carried, "seq", split_axis=0, concat_axis=0, tiled=True)
    gc, rows, end = pl.pallas_call(
        forward_kernel,
        grid=(4,),
        in_specs=[
            quarter, narrow, states, narrow,
            *[pl.BlockSpec((2, 32, 128), lambda g: (g, 0, 0))] * 4, narrow,
        ],
        out_specs=[narrow, rows8, state],
        out_shape=(
            shape(tok, 128), shape(4, 8, tok), shape(4, 128, 256),
        ),
        scratch_shapes=[
            pltpu.VMEM((256, 128), f32), pltpu.VMEM((tok, 256), f32)
        ],
        compiler_params=arbitrary,
        cost_estimate=cost(3 * 10**9, 10**7),
        name="forward",
    )(out_grad, c_proj, into, scales, *shifted, gc)
    gc = lax.all_to_all(
        gc.reshape(4, tok // 4, 128), "head", split_axis=0, concat_axis=0, tiled=True
    ).sum(axis=0)
    through, *gbs = pl.pallas_call(
        backward_kernel,
        grid=(4,),
        in_specs=[
            quarter, narrow, states, narrow, state,
            pl.BlockSpec((16, 1, 16, 128), lambda g: (0, g // 2, g % 2, 0)),
        ],
        out_specs=[pl.BlockSpec((1, 8, 128), lambda g: (g, 0, 0))] + [whole((tok // 4, 128))] * 4,
        out_shape=[shape(4, 8, 128)] + [shape(tok // 4, 128)] * 4,
        scratch_shapes=[pltpu.VMEM((tok, 128), f32), pltpu.VMEM((tok, 256), f32)],
        compiler_params=arbitrary,
        cost_estimate=cost(3 * 10**9, 10**7),
        name="backward",
    )(inputs, scales, back, gb, end, incoming.reshape(16, 2, 32, 128))
    moved = []
    for d, part in enumerate(gbs):
        moved.append(around(part, d))
    grad_inputs, grad_step_raw = pl.pallas_call(
        last_kernel,
        grid=(4,),
        in_specs=[
            quarter, narrow, narrow, whole((4, 24, tok)), block, rows8, rows8, states,
            pl.BlockSpec((16, 1, 16, 128), lambda g: (0, g // 2, g % 2, 0)),
            whole((4, 8, 128)),
        ],
        out_specs=[quarter, whole((16, tok))],
        out_shape=[shape(tok, 1024, dtype=bf16), shape(16, tok)],
        scratch_shapes=[pltpu.VMEM((4, 8, tok), f32), pltpu.VMEM((tok, 256), f32)],
        compiler_params=arbitrary,
        cost_estimate=cost(3 * 10**9, 10**7),
        name="last",
    )(
        inputs, b_proj, scales, info, adj, pair_rows, rows, back,
        incoming.reshape(16, 2, 32, 128), through,
    )
    gb = moved[0] + moved[1] + moved[3] + moved[2]
    return grad_inputs, grad_step_raw.T, gb, gc


def solution(mesh):
    return jax.shard_map(
        on_device,
        mesh=mesh,
        in_specs=(
            P("seq", "head"),
            P("seq", "head"),
            P("seq", None),
            P("seq", None),
            P("seq", "head"),
            P("head"),
            P("head"),
            P("head"),
            P(None, "seq", "head", None),
            P(),
        ),
        out_specs=(P("seq", "head"), P("seq", "head"), P(("seq", "head"), None), P(("seq", "head"), None)),
        check_vma=False,
    )
```

```python
import jax
import jax.numpy as jnp
from jax import lax
from jax.experimental import pallas as pl
from jax.experimental.pallas import tpu as pltpu
from jax.sharding import PartitionSpec as P

f32 = jnp.float32
bf16 = jnp.bfloat16
Q = 128
LOG2E = 1.4426950408889634
HIGHEST = lax.Precision.HIGHEST


def dn(a, b, precision=None):
    return lax.dot_general(
        a, b, (((1,), (0,)), ((), ())), precision=precision, preferred_element_type=f32
    )


def dt(a, b, precision=None):
    return lax.dot_general(
        a, b, (((1,), (1,)), ((), ())), precision=precision, preferred_element_type=f32
    )


def split(value):
    high = value.astype(bf16)
    low = (value - high.astype(f32)).astype(bf16)
    return high, low


def side(*parts):
    return jnp.concatenate(parts, axis=1)


def stack(*parts):
    return jnp.concatenate(parts, axis=0)


def spread(cols, base):
    rows = cols.shape[0]
    first = lax.broadcasted_iota(jnp.int32, (rows, 128), 1) < 64
    parts = []
    for j in range(2):
        left, right = (
            jnp.broadcast_to(cols[:, k : k + 1], (rows, 128))
            for k in (base + 2 * j, base + 2 * j + 1)
        )
        parts.append(jnp.where(first, left, right))
    return side(*parts)


def group_cols(cols, group):
    return pltpu.roll(cols, (128 - 4 * group) % 128, 1)


def head_sums(product):
    rows = []
    for j in range(2):
        turned = product[:, 128 * j : 128 * j + 128].T
        for i in range(2):
            part = turned[64 * i : 64 * i + 64]
            eight = part[0:8]
            for r in range(1, 8):
                eight = eight + part[8 * r : 8 * r + 8]
            rows.append(jnp.sum(eight, axis=0, keepdims=True))
    return stack(*rows)


GROW, SHRINK, GROW_ALL = 0, 32, 64
LOGCOL, SKIP = 0, 16


def repeater(base, group):
    row = lax.broadcasted_iota(jnp.int32, (128, 256), 0) - (base + 4 * group)
    head = lax.broadcasted_iota(jnp.int32, (128, 256), 1) // 64
    return jnp.where((row == head) | (row == head + 16), 1.0, 0.0).astype(bf16)


def first_kernel(
    slot_ref, raw_ref, rate_ref, bias_ref, skip_ref, dy_ref, c_ref, saved_ref,
    sums_ref, scales_ref, info_ref,
    pad_ref, ct_ref,
):
    g = pl.program_id(0)
    blocks = dy_ref.shape[0] // Q

    @pl.when(g == 0)
    def prepare():
        for k in range(saved_ref.shape[0]):
            sums_ref[slot_ref[k], 40:72, :] = saved_ref[k]
        pad_ref[0:8, 0:16] = jnp.broadcast_to(jnp.exp(rate_ref[...]), (8, 16))
        pad_ref[8:16, 0:16] = jnp.broadcast_to(bias_ref[...], (8, 16))
        pad_ref[16:24, 0:16] = jnp.broadcast_to(skip_ref[...], (8, 16))
        small = pad_ref[...].T
        rate, bias, skip = (
            jnp.broadcast_to(small[0:16, k : k + 1], (16, Q)) for k in (0, 8, 16)
        )
        row = lax.broadcasted_iota(jnp.int32, (Q, Q), 0)
        lane = lax.broadcasted_iota(jnp.int32, (Q, Q), 1)
        upper = jnp.where(row <= lane, 1.0, 0.0)
        steps, gates, decays = [], [], []
        for k in range(blocks):
            z = raw_ref[:, k * Q : (k + 1) * Q] + bias
            small_exp = jnp.exp(-jnp.abs(z))
            step = jnp.maximum(z, 0.0) + jnp.log1p(small_exp)
            gates.append(jnp.where(z >= 0.0, 1.0, small_exp) / (1.0 + small_exp))
            steps.append(step)
            decays.append(-rate * step * LOG2E)
        sums = dn(stack(*decays), upper, HIGHEST)
        logs = [sums[16 * k : 16 * k + 16] for k in range(blocks)]
        ends = [log[:, Q - 1 : Q] for log in logs]
        so_far = jnp.zeros_like(ends[0])
        fill = jnp.zeros((32, Q), f32)
        for k in range(blocks):
            log, step = logs[k], steps[k]
            parts = []
            for part in (
                jnp.exp2(log), step * jnp.exp2(ends[k] - log), jnp.exp2(log + so_far)
            ):
                high = part.astype(bf16).astype(f32)
                parts += [high, part - high]
            scales_ref[k * Q : (k + 1) * Q, :] = stack(*parts, fill).T.astype(bf16)
            so_far = so_far + ends[k]
            for r in range(4):
                four = slice(4 * r, 4 * r + 4)
                info_ref[r, :, k * Q : (k + 1) * Q] = stack(
                    log[four], step[four], gates[k][four], rate[four], skip[four], skip[four]
                )
            ct_ref[k] = c_ref[k * Q : (k + 1) * Q, :].astype(f32).T.astype(bf16)
        ends_row = []
        for r in range(4):
            last = dn(scales_ref[blocks * Q - 16 : blocks * Q, :], repeater(GROW_ALL, r))
            ends_row += [last[15:16, 0:128], last[15:16, 128:256]]
        for half in range(2):
            tile = stack(*ends_row[4 * half : 4 * half + 4], jnp.zeros((4, 128), f32))
            for i in range(16):
                sums_ref[2 * i + half, 32:40, :] = tile

    total = jnp.zeros((128, 256), f32)
    before = None
    grow_to = repeater(GROW, g)
    for k in range(blocks):
        rows = slice(k * Q, (k + 1) * Q)
        grow = dn(scales_ref[rows, :], grow_to)
        high, low = split(dy_ref[rows, :].astype(f32) * grow)
        ct = ct_ref[k]
        delta = dn(side(ct, ct), stack(high, low))
        end = grow[Q - 1 : Q, :]
        total = delta if k == 0 else total + before * delta
        before = end if k == 0 else before * end
    at = pl.ds(pl.multiple_of((g % 2) * 16, 16), 16)
    for i in range(16):
        part = total[8 * i : 8 * i + 8]
        sums_ref[2 * i + g // 2, at, :] = stack(part[:, 0:128], part[:, 128:256])


def carry_kernel(sums_ref, out_ref, *start_refs):
    here = lax.axis_index("head")
    for d in range(4):
        group = lax.rem(here + d, 4)
        start_refs[d][...] = sums_ref[pl.ds(pl.multiple_of(group * 8, 8), 8), 40:72, :]
    carried = [jnp.zeros((8, 128), f32) for _ in range(4)]
    for m in reversed(range(sums_ref.shape[0])):
        for r in range(4):
            tile = slice(8 * r, 8 * r + 8)
            out_ref[m, tile, :] = carried[r]
            decay = jnp.broadcast_to(sums_ref[m, 32 + r : 33 + r, :], (8, 128))
            carried[r] = sums_ref[m, tile, :] + decay * carried[r]


def pair_kernel(
    x_ref, dy_ref, b_ref, c_ref, scales_ref, info_ref,
    adj_ref, rows_ref, into_ref, back_ref, xhigh_ref, xlow_ref, dyhigh_ref, dylow_ref, decay_ref,
    gb_ref, gc_ref,
    tot_ref, meet_ref, scale_ref, cols_ref, bt_ref, ct_ref,
):
    g = pl.program_id(0)
    blocks = x_ref.shape[0] // Q

    @pl.when(g == 0)
    def clear():
        for k in range(blocks):
            rows = slice(k * Q, (k + 1) * Q)
            meet_ref[k] = dt(b_ref[rows, :], c_ref[rows, :])
            ct_ref[k] = c_ref[rows, :].astype(f32).T.astype(bf16)
            bt_ref[k] = b_ref[rows, :].astype(f32).T.astype(bf16)
            logs = [
                info_ref[r, 0:4, rows] - jnp.log(info_ref[r, 4:8, rows]) * LOG2E for r in range(4)
            ]
            skips = [info_ref[r, 16:20, rows] for r in range(4)]
            cols_ref[rows, :] = stack(*logs, *skips, jnp.zeros((96, Q), f32)).T
        tot_ref[...] = jnp.zeros_like(tot_ref)

    skip = spread(group_cols(cols_ref[0:8, :], g), SKIP)[0:1, :]
    for source_ref, base, turn_ref, out_ref, high_ref, low_ref in (
        (x_ref, SHRINK, bt_ref, into_ref, xhigh_ref, xlow_ref),
        (dy_ref, GROW, ct_ref, back_ref, dyhigh_ref, dylow_ref),
    ):
        scale_ref[...] = dn(scales_ref[...], repeater(base, g))
        for k in range(blocks):
            rows = slice(k * Q, (k + 1) * Q)
            high, low = split(source_ref[rows, :].astype(f32) * scale_ref[rows, :])
            high_ref[0, rows, :] = high
            low_ref[0, rows, :] = low
            turn = turn_ref[k]
            out_ref[0, k] = dn(side(turn, turn), stack(high, low))
    decay_ref[0] = stack(*[scale_ref[k * Q + Q - 1 : k * Q + Q, :] for k in range(blocks)])

    upper = lax.broadcasted_iota(jnp.int32, (Q, Q), 0) <= lax.broadcasted_iota(
        jnp.int32, (Q, Q), 1
    )
    lane = lax.broadcasted_iota(jnp.int32, (1, 128), 1)
    masks = [
        jnp.where(lane < 64, 1.0, 0.0).astype(bf16),
        jnp.where(lane < 64, 0.0, 1.0).astype(bf16),
    ]

    def one(k):
        rows = pl.ds(pl.multiple_of(k * Q, Q), Q)
        cols = group_cols(cols_ref[rows, :], g)
        meet = meet_ref[k]
        total = tot_ref[k]
        in_rows, products = [], []
        for j in range(2):
            lanes = slice(128 * j, 128 * j + 128)
            x_pair, dy_pair = x_ref[rows, lanes], dy_ref[rows, lanes]
            dots = dt(stack(x_pair * masks[0], x_pair * masks[1]), dy_pair)
            weights, values = [], []
            for i in range(2):
                h = 2 * j + i
                gap = info_ref[g, h : h + 1, rows] - jnp.broadcast_to(
                    cols[:, LOGCOL + h : LOGCOL + h + 1], (Q, Q)
                )
                decay = jnp.exp2(jnp.where(upper, gap, -1e30))
                pair = dots[Q * i : Q * i + Q] * decay
                total = total + pair
                in_rows.append(jnp.sum(pair * meet, axis=0, keepdims=True))
                weights += list(split(decay * meet))
                values += [dy_pair * masks[i]] * 2
            adj = dn(side(*weights), stack(*values))
            adj_ref[0, rows, lanes] = adj + skip[:, lanes] * dy_pair.astype(f32)
            products.append(x_pair.astype(f32) * adj)
        tot_ref[k] = total
        rows_ref[0, 0:4, rows] = stack(*in_rows)
        rows_ref[0, 4:8, rows] = head_sums(side(*products))

    def some(i, unused):
        for k in range(PAIR_UNROLL):
            one(i * PAIR_UNROLL + k)
        return unused

    lax.fori_loop(0, blocks // PAIR_UNROLL, some, 0)

    @pl.when(g == pl.num_programs(0) - 1)
    def finish():
        for k in range(blocks):
            rows = slice(k * Q, (k + 1) * Q)
            total = tot_ref[k]
            high, low = split(total)
            c = c_ref[rows, :]
            gb_ref[rows, :] = dn(side(high, low), stack(c, c))
            high, low = split(total.T)
            b = b_ref[rows, :]
            gc_ref[rows, :] = dn(side(high, low), stack(b, b))


PAIR_UNROLL = 8


def three(rows_high, rows_low, high, low):
    both = dt(rows_high, stack(high, low))
    return both[:, 0:128] + both[:, 128:256] + dt(rows_low, high)


def forward_kernel(
    dyhigh_ref, dylow_ref, c_ref, into_ref, decay_ref, start0_ref, start1_ref, start2_ref, start3_ref, gc_in_ref,
    gc_ref, rows_ref, end_ref,
    hold_ref,
):
    g = pl.program_id(0)
    blocks = c_ref.shape[0] // Q

    @pl.when(g == 0)
    def copy():
        gc_ref[...] = gc_in_ref[...]

    here = lax.axis_index("head")
    for d, start_ref in enumerate((start0_ref, start1_ref, start2_ref, start3_ref)):
        part = lax.rem(here + 4 - d, 4)
        for h in range(4):
            at = 16 * (h % 2)
            to = pl.ds(pl.multiple_of(64 * h + 16 * part, 16), 16)
            hold_ref[to, :] = start_ref[h // 2, at : at + 16, :]
    state = hold_ref[...].T
    for k in range(blocks):
        rows = slice(k * Q, (k + 1) * Q)
        s_high, s_low = split(state)
        c = c_ref[rows, :]
        from_state = dn(side(c, c), stack(s_high, s_low))
        dy_high, dy_low = dyhigh_ref[0, rows, :], dylow_ref[0, rows, :]
        dy_grown = dy_high.astype(f32) + dy_low.astype(f32)
        rows_ref[0, 0:4, rows] = head_sums(dy_grown * from_state)
        gc_ref[rows, :] += three(dy_high, dy_low, s_high, s_low)
        state = decay_ref[0, k : k + 1, :] * state + into_ref[0, k]
    end_ref[0] = state


def backward_kernel(
    xhigh_ref, xlow_ref, decay_ref, back_ref, gb_in_ref, end_ref, in_ref,
    through_ref, gb0_ref, gb1_ref, gb2_ref, gb3_ref,
    gb_ref,
):
    g = pl.program_id(0)
    blocks = gb_ref.shape[0] // Q

    @pl.when(g == 0)
    def copy():
        gb_ref[...] = gb_in_ref[...]

    adjoint = side(*[in_ref[:, 0, 8 * r : 8 * r + 8, :].reshape(128, 128) for r in range(2)])
    meeting = jnp.sum(adjoint * end_ref[0], axis=0, keepdims=True)
    row = lax.broadcasted_iota(jnp.int32, (8, 256), 0)
    lane = lax.broadcasted_iota(jnp.int32, (8, 256), 1)
    through = jnp.sum(jnp.where(row == lane // 64, meeting, 0.0), axis=1, keepdims=True)
    through_ref[0] = jnp.broadcast_to(through, (8, 128))
    for k in reversed(range(blocks)):
        rows = slice(k * Q, (k + 1) * Q)
        x_high, x_low = xhigh_ref[0, rows, :], xlow_ref[0, rows, :]
        g_high, g_low = split(adjoint)
        gb_ref[rows, :] += three(x_high, x_low, g_high, g_low)
        adjoint = decay_ref[0, k : k + 1, :] * adjoint + back_ref[0, k]

    @pl.when(g == pl.num_programs(0) - 1)
    def finish():
        here = lax.axis_index("head")
        for d, part_ref in enumerate((gb0_ref, gb1_ref, gb2_ref, gb3_ref)):
            size = part_ref.shape[0]
            at = lax.rem(here + d, 4) * size
            part_ref[...] = gb_ref[pl.ds(pl.multiple_of(at, size), size), :]


def last_kernel(
    x_ref, b_ref, scales_ref, info_ref, adj_ref, pair_rows_ref, rows_ref,
    back_ref, decay_ref, in_ref, through_ref,
    gx_ref, raw_ref,
    keep_ref, shrink_ref,
):
    g = pl.program_id(0)
    blocks = x_ref.shape[0] // Q
    adjoint = side(*[in_ref[:, 0, 8 * r : 8 * r + 8, :].reshape(128, 128) for r in range(2)])
    shrink_ref[...] = dn(scales_ref[...], repeater(SHRINK, g))
    for k in reversed(range(blocks)):
        rows = slice(k * Q, (k + 1) * Q)
        b = b_ref[rows, :]
        adj = shrink_ref[rows, :] * dn(side(b, b), stack(*split(adjoint)))
        adjoint = decay_ref[0, k : k + 1, :] * adjoint + back_ref[0, k]
        gx_ref[rows, :] = (adj_ref[0, rows, :] + adj).astype(bf16)
        out_rows = pair_rows_ref[0, 4:8, rows] + head_sums(x_ref[rows, :].astype(f32) * adj)
        keep_ref[g, 0:4, rows] = (
            pair_rows_ref[0, 0:4, rows] + rows_ref[0, 0:4, rows] - out_rows
        )
        keep_ref[g, 4:8, rows] = out_rows

    @pl.when(g == pl.num_programs(0) - 1)
    def finish():
        after = jnp.where(
            lax.broadcasted_iota(jnp.int32, (Q, Q), 0)
            >= lax.broadcasted_iota(jnp.int32, (Q, Q), 1),
            1.0, 0.0,
        )

        def all_heads(ref, first, rows):
            return stack(*[ref[r, first : first + 4, rows] for r in range(4)])

        parts = [all_heads(keep_ref, 0, slice(k * Q, (k + 1) * Q)) for k in range(blocks)]
        sums = dn(stack(*parts), after, HIGHEST)
        later = stack(*[through_ref[r, 0:4, 0:1] for r in range(4)])
        for k in reversed(range(blocks)):
            rows = slice(k * Q, (k + 1) * Q)
            here = sums[16 * k : 16 * k + 16]
            step, gate, rate = (all_heads(info_ref, 4 * r, rows) for r in (1, 2, 3))
            x_adj = all_heads(keep_ref, 4, rows)
            raw_ref[:, rows] = gate * (x_adj / step - rate * (here + later))
            later = later + here[:, 0:1]


def whole(shape):
    zeros = (0,) * len(shape)
    return pl.BlockSpec(tuple(shape), lambda g, zeros=zeros: zeros)


def around(array, distance):
    if distance == 0:
        return array
    heads = lax.axis_size("head")
    return lax.ppermute(array, "head", [(i, (i + distance) % heads) for i in range(heads)])


def on_device(
    inputs, out_grad, b_proj, c_proj, step_raw, log_rate, step_bias, skip_gain,
    saved_states, segment_slot,
):
    tok = inputs.shape[0]
    blocks = tok // Q
    segs = saved_states.shape[0]
    arbitrary = pltpu.CompilerParams(dimension_semantics=("arbitrary",))

    def shape(*dims, dtype=f32):
        return jax.ShapeDtypeStruct(dims, dtype)

    def cost(flops, bytes_accessed):
        return pl.CostEstimate(
            flops=flops, transcendentals=0, bytes_accessed=bytes_accessed
        )

    quarter = pl.BlockSpec((tok, 256), lambda g: (0, g))
    narrow = whole((tok, 128))
    rows8 = pl.BlockSpec((1, 8, tok), lambda g: (g, 0, 0))
    states = pl.BlockSpec((1, blocks, 128, 256), lambda g: (g, 0, 0, 0))
    block = pl.BlockSpec((1, tok, 256), lambda g: (g, 0, 0))
    ends = pl.BlockSpec((1, blocks, 256), lambda g: (g, 0, 0))
    state = pl.BlockSpec((1, 128, 256), lambda g: (g, 0, 0))
    sums, scales, info = pl.pallas_call(
        first_kernel,
        grid=(4,),
        in_specs=[
            pl.BlockSpec(memory_space=pltpu.SMEM), whole((16, tok)), whole((1, 16)),
            whole((1, 16)), whole((1, 16)), quarter, narrow, whole((segs, 32, 128)),
        ],
        out_specs=[whole((segs, 72, 128)), narrow, whole((4, 24, tok))],
        out_shape=(
            shape(segs, 72, 128), shape(tok, 128, dtype=bf16), shape(4, 24, tok),
        ),
        scratch_shapes=[pltpu.VMEM((128, 128), f32), pltpu.VMEM((blocks, 128, Q), bf16)],
        compiler_params=arbitrary,
        cost_estimate=cost(10**9, 10**7),
        name="first",
    )(
        segment_slot, step_raw.T, log_rate[None], step_bias[None], skip_gain[None], out_grad,
        c_proj, saved_states.reshape(segs, 32, 128),
    )
    sums = lax.all_to_all(sums, "seq", split_axis=0, concat_axis=0, tiled=True)

    adj, pair_rows, into, back, x_high, x_low, dy_high, dy_low, decays, gb, gc = pl.pallas_call(
        pair_kernel,
        grid=(4,),
        in_specs=[
            quarter, quarter, narrow, narrow, narrow, whole((4, 24, tok))
        ],
        out_specs=[block, rows8, states, states] + [block] * 4 + [ends, narrow, narrow],
        out_shape=[
            shape(4, tok, 256), shape(4, 8, tok), shape(4, blocks, 128, 256),
            shape(4, blocks, 128, 256), *[shape(4, tok, 256, dtype=bf16)] * 4,
            shape(4, blocks, 256), shape(tok, 128), shape(tok, 128),
        ],
        scratch_shapes=[
            pltpu.VMEM((blocks, Q, Q), f32), pltpu.VMEM((blocks, Q, Q), f32),
            pltpu.VMEM((tok, 256), f32), pltpu.VMEM((tok, 128), f32),
            pltpu.VMEM((blocks, 128, Q), bf16), pltpu.VMEM((blocks, 128, Q), bf16),
        ],
        compiler_params=arbitrary,
        cost_estimate=cost(2 * 10**10, 10**7),
        name="pairs",
    )(inputs, out_grad, b_proj, c_proj, scales, info)
    sums, gb = lax.optimization_barrier((sums, gb))
    carried, *starts = pl.pallas_call(
        carry_kernel,
        grid=(1,),
        in_specs=[whole((segs, 72, 128))],
        out_specs=[whole((segs, 32, 128))] + [whole((8, 32, 128))] * 4,
        out_shape=[pltpu.HBM((segs, 32, 128), f32)] + [pltpu.HBM((8, 32, 128), f32)] * 4,
        compiler_params=pltpu.CompilerParams(vmem_limit_bytes=8 * 2**20),
        cost_estimate=cost(10**6, 10**6),
        name="carry",
    )(sums)
    shifted = []
    for d, start in enumerate(starts):
        shifted.append(around(start, d))
    incoming = lax.all_to_all(carried, "seq", split_axis=0, concat_axis=0, tiled=True)
    gc, rows, end = pl.pallas_call(
        forward_kernel,
        grid=(4,),
        in_specs=[
            block, block, narrow, states, ends,
            *[pl.BlockSpec((2, 32, 128), lambda g: (g, 0, 0))] * 4, narrow,
        ],
        out_specs=[narrow, rows8, state],
        out_shape=(
            shape(tok, 128), shape(4, 8, tok), shape(4, 128, 256),
        ),
        scratch_shapes=[
            pltpu.VMEM((256, 128), f32),
        ],
        compiler_params=arbitrary,
        cost_estimate=cost(3 * 10**9, 10**7),
        name="forward",
    )(dy_high, dy_low, c_proj, into, decays, *shifted, gc)
    gc = lax.all_to_all(
        gc.reshape(4, tok // 4, 128), "head", split_axis=0, concat_axis=0, tiled=True
    ).sum(axis=0)
    through, *gbs = pl.pallas_call(
        backward_kernel,
        grid=(4,),
        in_specs=[
            block, block, ends, states, narrow, state,
            pl.BlockSpec((16, 1, 16, 128), lambda g: (0, g // 2, g % 2, 0)),
        ],
        out_specs=[pl.BlockSpec((1, 8, 128), lambda g: (g, 0, 0))] + [whole((tok // 4, 128))] * 4,
        out_shape=[shape(4, 8, 128)] + [shape(tok // 4, 128)] * 4,
        scratch_shapes=[pltpu.VMEM((tok, 128), f32)],
        compiler_params=arbitrary,
        cost_estimate=cost(3 * 10**9, 10**7),
        name="backward",
    )(x_high, x_low, decays, back, gb, end, incoming.reshape(16, 2, 32, 128))
    moved = []
    for d, part in enumerate(gbs):
        moved.append(around(part, d))
    grad_inputs, grad_step_raw = pl.pallas_call(
        last_kernel,
        grid=(4,),
        in_specs=[
            quarter, narrow, narrow, whole((4, 24, tok)), block, rows8, rows8, states, ends,
            pl.BlockSpec((16, 1, 16, 128), lambda g: (0, g // 2, g % 2, 0)),
            whole((4, 8, 128)),
        ],
        out_specs=[quarter, whole((16, tok))],
        out_shape=[shape(tok, 1024, dtype=bf16), shape(16, tok)],
        scratch_shapes=[pltpu.VMEM((4, 8, tok), f32), pltpu.VMEM((tok, 256), f32)],
        compiler_params=arbitrary,
        cost_estimate=cost(3 * 10**9, 10**7),
        name="last",
    )(
        inputs, b_proj, scales, info, adj, pair_rows, rows, back, decays,
        incoming.reshape(16, 2, 32, 128), through,
    )
    gb = moved[0] + moved[1] + moved[3] + moved[2]
    return grad_inputs, grad_step_raw.T, gb, gc


def solution(mesh):
    return jax.shard_map(
        on_device,
        mesh=mesh,
        in_specs=(
            P("seq", "head"),
            P("seq", "head"),
            P("seq", None),
            P("seq", None),
            P("seq", "head"),
            P("head"),
            P("head"),
            P("head"),
            P(None, "seq", "head", None),
            P(),
        ),
        out_specs=(P("seq", "head"), P("seq", "head"), P(("seq", "head"), None), P(("seq", "head"), None)),
        check_vma=False,
    )
```
